256 devices in a mesh: rep: 2 (over core), dp: 128 (over x, y, z).
Axes of the slice: x: 4, y: 4, z: 8, core: 2. Of those that a mesh axis runs over, the one named last changes fastest.
Arguments:
- x: bfloat16 [256, 2048, 1024], P(('rep', 'dp')), parts along dimension 0
- dy: bfloat16 [256, 2048, 1024], P(('rep', 'dp')), parts along dimension 0
- w_gate: bfloat16 [2, 1024, 2816], replicated
- w_up: bfloat16 [2, 1024, 2816], replicated
- w_down: bfloat16 [2, 2816, 1024], replicated
- m_w_gate: float32 [2, 1024, 2816], P(None, 'dp')
- m_w_up: float32 [2, 1024, 2816], P(None, 'dp')
- m_w_down: float32 [2, 2816, 1024], P(None, 'dp')
- v_w_gate: float32 [2, 1024, 2816], P(None, 'dp')
- v_w_up: float32 [2, 1024, 2816], P(None, 'dp')
- v_w_down: float32 [2, 2816, 1024], P(None, 'dp')
Outputs:
- output 1: bfloat16 [4, 1024, 2816], P('rep'), parts along dimension 0
- output 2: bfloat16 [4, 1024, 2816], P('rep'), parts along dimension 0
- output 3: bfloat16 [4, 2816, 1024], P('rep'), parts along dimension 0
- output 4: float32 [4, 1024, 2816], P('rep', 'dp'), parts along dimension 0
- output 5: float32 [4, 1024, 2816], P('rep', 'dp'), parts along dimension 0
- output 6: float32 [4, 2816, 1024], P('rep', 'dp'), parts along dimension 0
- output 7: float32 [4, 1024, 2816], P('rep', 'dp'), parts along dimension 0
- output 8: float32 [4, 1024, 2816], P('rep', 'dp'), parts along dimension 0
- output 9: float32 [4, 2816, 1024], P('rep', 'dp'), parts along dimension 0
There are 2 independent parts. The reference program is written for one: setup_inputs(seed, part) draws one part's arguments, and reference() takes and returns one part's arrays. A program takes and returns all parts, laid end to end along the dimension named above; an argument that names none is the same for every part.
All inputs are finite; a program needn't handle non-finite values.
Results may differ from the reference program's by a relative error of at most 0.022.
Values are sent between devices in bfloat16 or wider.
A program may use at most 768 MiB of HBM per device.

```python
import jax
import jax.numpy as jnp
from jax import lax

SEQUENCES = 128
TOKENS = 2048
D = 1024
FF = 2816
LAYERS = 2
NAMES = ("w_gate", "w_up", "w_down")
SHAPES = {"w_gate": (LAYERS, D, FF), "w_up": (LAYERS, D, FF), "w_down": (LAYERS, FF, D)}


def bump(key, n, height):
    away = (jnp.arange(n, dtype=jnp.int32) - jax.random.randint(key, (), 0, n, jnp.int32)) % n
    return jnp.where(away < n // 8, height, 1.0)


def together(key, own, strength):
    shared = jax.random.normal(key, own.shape[1:], jnp.float32)
    return (own + strength * shared) * lax.rsqrt(1 + strength * strength)


def setup_inputs(seed: int = 0, part: int = 0) -> dict:
    kx, kdy, ka, kb, kz, kf, kh, kl, *keys = jax.random.split(jax.random.key(seed), 8 + 3 * len(NAMES))
    kx, kdy, ka, kb = (jax.random.fold_in(k, part) for k in (kx, kdy, ka, kb))
    kw, km, kv = (keys[i::3] for i in range(3))
    shape = (SEQUENCES, TOKENS, D)
    much_x, much_dy = jax.random.uniform(kz, (2,), jnp.float32, 0.0, 1.0)
    loud = 2.0 ** jax.random.uniform(jax.random.fold_in(kz, 1), (), jnp.float32, -1.0, 2.0)
    layers = 2.0 ** jax.random.uniform(kl, (LAYERS, 1, 1), jnp.float32, -1.0, 1.0)
    x = together(ka, jax.random.normal(kx, shape, jnp.float32), much_x) * bump(kf, D, 4.0)
    dy = together(kb, jax.random.normal(kdy, shape, jnp.float32), much_dy)
    drawn = {"x": x.astype(jnp.bfloat16), "dy": (loud * dy * (SEQUENCES * TOKENS) ** -0.5).astype(jnp.bfloat16)}
    for key, name in zip(kw, NAMES, strict=True):
        w = jax.random.normal(key, SHAPES[name], jnp.float32) * SHAPES[name][1] ** -0.5
        drawn[name] = (w * {"w_gate": 1.0, "w_up": bump(kh, FF, 4.0), "w_down": layers}[name]).astype(jnp.bfloat16)
    for key, name in zip(km, NAMES, strict=True):
        drawn[f"m_{name}"] = 0.1 * jax.random.normal(key, SHAPES[name], jnp.float32)
    for key, name in zip(kv, NAMES, strict=True):
        drawn[f"v_{name}"] = loud * loud * jax.random.uniform(key, SHAPES[name], jnp.float32, 0.05, 0.15)
    return drawn


def matmul(a, w):
    return jnp.dot(a, w, preferred_element_type=jnp.float32).astype(jnp.bfloat16)


def normed(h):
    wide = h.astype(jnp.float32)
    scale = lax.rsqrt(jnp.mean(wide**2, -1, keepdims=True) + 1e-6)
    return (wide * scale).astype(jnp.bfloat16)


def layer(h, w):
    a = normed(h)
    gate = jnp.dot(a, w["w_gate"], preferred_element_type=jnp.float32)
    up = jnp.dot(a, w["w_up"], preferred_element_type=jnp.float32)
    return h + matmul((jax.nn.silu(gate) * up).astype(jnp.bfloat16), w["w_down"])


def adamw(w, m, v, g):
    m = 0.9 * m + 0.1 * g
    v = 0.95 * v + 0.05 * g * g
    step = m * lax.rsqrt(v + 1e-8) + 0.1 * w
    return (w - 0.02 * step).astype(jnp.bfloat16), m, v


def stack(weights, h):
    return lax.scan(lambda h, w: (layer(h, w), None), h, weights)[0]


def reference(x, dy, w_gate, w_up, w_down, m_w_gate, m_w_up, m_w_down, v_w_gate, v_w_up, v_w_down):
    weights = dict(zip(NAMES, (w_gate, w_up, w_down), strict=True))

    def take(so_far, sequence):
        h, by_y = sequence
        _, back = jax.vjp(lambda w: stack(w, h), weights)
        return jax.tree.map(lambda total, term: total + term.astype(jnp.float32), so_far, back(by_y)[0]), None

    none_yet = {name: jnp.zeros(w.shape, jnp.float32) for name, w in weights.items()}
    by_weights, _ = lax.scan(take, none_yet, (x, dy))
    gradients = [by_weights[name].astype(jnp.bfloat16).astype(jnp.float32) for name in NAMES]
    new = [
        adamw(w.astype(jnp.float32), m, v, g)
        for w, m, v, g in zip((w_gate, w_up, w_down), (m_w_gate, m_w_up, m_w_down), (v_w_gate, v_w_up, v_w_down), gradients, strict=True)
    ]
    return tuple(one[which] for which in range(3) for one in new)
```

```python
import functools

import jax
import jax.numpy as jnp
from jax import lax
from jax.experimental import pallas as pl
from jax.experimental.pallas import tpu as pltpu

LOGICAL = pl.DeviceIdType.LOGICAL
F32, BF16 = jnp.float32, jnp.bfloat16
T, D, FF = 2048, 1024, 2816
SIZE = {"x": 4, "y": 4, "z": 8}
STRIDE = {"x": 32, "y": 8, "z": 1}
PARTNERS = 13
MESSAGES = 39


class Place:
    def __init__(self):
        me = lax.axis_index("dp")
        self.at = {"x": me // 32, "y": (me // 8) % 4, "z": me % 8}
        self.number = lax.axis_index("rep") * 128 + me
        self.ring = {(axis, step): (self.at_step(axis, step), self.partner(axis, step)) for axis in "xyz" for step in (1, -1)}

    def at_step(self, axis, step):
        return lax.rem(self.at[axis] + (step + SIZE[axis] if isinstance(step, int) else step), SIZE[axis])

    def chunk(self, axis, step):
        return self.at[axis] if isinstance(step, int) and step == 0 else self.at_step(axis, step)

    def partner(self, axis, step):
        return self.number + (self.at_step(axis, step) - self.at[axis]) * STRIDE[axis]

    def tell(self, semaphore):
        for axis, n in SIZE.items():

            def one(step, c, axis=axis):
                pl.semaphore_signal(semaphore, inc=1, device_id=self.partner(axis, step), device_id_type=LOGICAL)
                return c

            lax.fori_loop(1, n, one, 0)

    def greet(self):
        barrier = pltpu.get_barrier_semaphore()
        self.tell(barrier)
        pl.semaphore_wait(barrier, PARTNERS)


class Action:
    def __init__(self, waits, do, sends, cost=0.3, frees=False):
        self.waits, self.do, self.sends, self.cost, self.frees = waits, do, sends, cost, frees


class Chain:
    def __init__(self, actions, release, before=None):
        self.actions, self.release, self.before, self.done, self.freed = actions, release, before, 0, None

    def ended(self):
        return self.done == len(self.actions)


RATE = 46.0e3


def plan(chains, ticks, latency=3.0):
    free, arrive, now, placed, rest = {}, {}, 0.0, [], []

    def run(c, a, at):
        if a.frees:
            c.freed = at
        for name, link, nbytes, further in a.sends:
            begin = max(free.get(link, 0.0), at + a.cost)
            free[link] = begin + nbytes / RATE
            arrive[name] = free[link] + latency + further

    def ready(c, tick):
        if c.ended() or c.release > tick or (c.before and c.before.freed is None):
            return None
        waits = c.actions[c.done].waits
        known = [arrive[w] for w in waits if w in arrive] + [c.before.freed + latency if c.before else 0.0]
        return max(known) if len(known) > len(waits) else None

    for tick, time in enumerate(ticks):
        now += time
        here = []
        while True:
            best = min(((r, i) for i, c in enumerate(chains) if (r := ready(c, tick)) is not None and r <= now), default=None)
            if best is None:
                break
            c = chains[best[1]]
            a = c.actions[c.done]
            c.done += 1
            run(c, a, now)
            now += a.cost
            here.append(a)
        placed.append(here)
    while not all(c.ended() for c in chains):
        r, i = min((max(r, now - 1e3), i) for i, c in enumerate(chains) if (r := ready(c, len(ticks))) is not None)
        c = chains[i]
        a = c.actions[c.done]
        c.done += 1
        now = max(r, now)
        run(c, a, now)
        now += a.cost
        rest.append(a)
    return placed, rest, now


def volume(shape):
    n = 2
    for v in shape:
        n *= v
    return n


def each(shape, f):
    if len(shape) > 3 or shape[-2] == 176 and len(shape) == 3:
        lax.fori_loop(0, shape[0], lambda i, c: (f((i,)), c)[1], 0)
    else:
        f((slice(None),) * len(shape))


class Strip:
    def __init__(self, kind, start, width, role, axes):
        self.kind, self.start, self.width, self.role, self.axes = kind, start, width, role, axes
        self.cols = pl.ds(start, width)
        left = [a for a in "xyz" if a != axes[0]]
        if kind == "down":
            shapes = ((4, 176), (176,), (24,))
        else:
            shapes = ((SIZE[left[0]], SIZE[left[1]], 8), (SIZE[left[1]], 8), (8,))
        self.shapes = [(*s, width) for s in shapes]
        self.back = axes[::-1]
        n = SIZE[axes[0]]
        self.far = {1: n // 2 if role == 0 else n // 2 - 1, -1: n // 2 if role == 1 else n // 2 - 1}
        self.ring = [(d, k) for d in (1, -1) for k in range(self.far[d], 0, -1)]
        self.counts = [SIZE[a] - 1 for a in (*axes, *self.back)]
        sums = {d: [d * k for k in range(self.far[d] - 1, 0, -1)] for d in (1, -1)}
        short = -1 if role == 0 else 1
        sums[short] = sums[short] + [0]
        self.own = [sums[-short] + sums[short]] if n == 4 else [sums[1], sums[-1]]

    def offset(self, layer, what, i):
        if what == "rs":
            return sum(self.counts[:i])
        return sum(self.counts[: 3 + i]) + layer * sum(self.counts[3:])

    def scratch(self):
        s = {"own": pltpu.VMEM((len(self.own), *self.shapes[0]), BF16), "acc1": pltpu.VMEM(self.shapes[1], F32)}
        s["acc2"] = pltpu.VMEM((SIZE[self.axes[2]], *self.shapes[2]), F32)
        for i in range(3):
            s[f"recv{i}"] = pltpu.VMEM((self.counts[i], *self.shapes[i]), BF16)
        for i in (1, 2):
            s[f"send{i}"] = pltpu.VMEM((self.counts[i], *self.shapes[i]), BF16)
        if self.kind == "down":
            s["flat"] = pltpu.VMEM(self.shapes[1], F32)
            s["blocks"] = pltpu.VMEM((2, 8, *self.shapes[2]), BF16)
            s["rows"] = pltpu.VMEM((2, *self.shapes[1]), BF16)
        return s

    def chain(self, place, layer, grad, new, out, refs, sems, update):
        send_sem, recv_sem, local_sem, free_sem, place_of = sems
        axes, back, shapes, cols = self.axes, self.back, self.shapes, self.cols
        base, first_local = place_of * MESSAGES, place_of * 6

        def name(*m):
            return (layer, id(self), *m)

        def raw(step):
            c = place.chunk(axes[0], step)
            if self.kind == "down":
                return grad.at[c, :, :, cols] if axes[0] == "x" else grad.at[:, c, :, cols]
            return grad.at[(*(c if a == axes[0] else slice(None) for a in "xyz"), slice(None), cols)]

        def received(d, k):
            return refs["recv0"].at[self.ring.index((d, k))]

        def source(d, k):
            return received(d, k + 1) if k < self.far[d] else raw(d * k)

        def part(i, step):
            c = place.chunk(back[i], step)
            if self.kind == "down" and i == 0:
                return refs["blocks"].at[layer, c]
            known = {a: (slice(None) if a in back[:i] else c if a == back[i] else place.chunk(a, 0)) for a in "xyz"}
            if self.kind == "down":
                return out.at[known["x"], known["y"], :, cols]
            return out.at[known["x"], known["y"], known["z"], :, cols]

        def like(what, i):
            return refs[f"recv{i}"].at[0] if what == "rs" else part(i, 0)

        def send(what, i, n, src, dst, device):
            n = base + self.offset(layer, what, i) + n
            pltpu.make_async_remote_copy(src, dst, send_sem.at[n], recv_sem.at[n], device_id=device, device_id_type=LOGICAL).start()

        def wait(sem, what, i, n):
            ref = like(what, i)
            pltpu.make_async_copy(ref, ref, sem.at[base + self.offset(layer, what, i) + n]).wait()

        def wait_all(sem, what, i):
            count = self.counts[i if what == "rs" else 3 + i]
            lax.fori_loop(0, count, lambda n, c: (wait(sem, what, i, n), c)[1], 0)

        def ring_send(d, k):
            send("rs", 0, self.ring.index((d, k)), source(d, k), received(d, k), place.ring[axes[0], d][1])

        def ring_back(d, k):
            there = part(2, -d * (k - 1))
            send("ag", 2, self.ring.index((d, k)), there, there, place.ring[back[2], d][1])

        def to_each(what, i, f):
            axis = (axes if what == "rs" else back)[i]

            def one(step, c):
                send(what, i, step - 1, *f(step), place.partner(axis, step))
                return c

            lax.fori_loop(1, SIZE[axis], one, 0)

        def own_copy(step):
            b = next(b for b, seq in enumerate(self.own) if step in seq)
            return pltpu.make_async_copy(raw(step), refs["own"].at[b], local_sem.at[first_local + b])

        def own(step):
            b = next(b for b, seq in enumerate(self.own) if step in seq)
            mine = refs["own"].at[b]
            pltpu.make_async_copy(mine, mine, local_sem.at[first_local + b]).wait()
            return mine

        def begin():
            if layer == 0:
                for i in (1, 2):
                    wait_all(send_sem, "rs", i)
                for d in (1, -1):
                    wait(send_sem, "rs", 0, self.ring.index((d, self.far[d])))
                pl.semaphore_wait(free_sem.at[place_of], PARTNERS)
            for d in (1, -1):
                ring_send(d, self.far[d])
            for seq in self.own:
                own_copy(seq[0]).start()

        def add(d, k):
            wait(recv_sem, "rs", 0, self.ring.index((d, k + 1)))
            theirs, mine = received(d, k + 1), own(d * k)

            def f(at):
                theirs[at] = (mine[at].astype(F32) + theirs[at].astype(F32)).astype(BF16)

            each(shapes[0], f)
            for seq in self.own:
                if d * k in seq[:-1]:
                    own_copy(seq[seq.index(d * k) + 1]).start()
            ring_send(d, k)

        def end_0():
            mine = own(0)
            for d in (1, -1):
                wait(recv_sem, "rs", 0, self.ring.index((d, 1)))

            def total(step):
                c = place.chunk(axes[1], step)
                return mine[c].astype(F32) + received(1, 1)[c].astype(F32) + received(-1, 1)[c].astype(F32)

            def f(step):
                to = refs["send1"].at[step - 1]
                to[...] = total(step).astype(BF16)
                return to, refs["recv1"].at[step - 1]

            to_each("rs", 1, f)
            refs["acc1"][...] = total(0)

        def end_1():
            wait_all(recv_sem, "rs", 1)
            acc2 = refs["acc2"]
            total = refs["acc1"][...]
            for n in range(self.counts[1]):
                total = total + refs["recv1"][n].astype(F32)
            if self.kind == "down":
                refs["flat"][...] = total
                for z in range(8):
                    acc2[z, :22, :] = refs["flat"][22 * z : 22 * z + 22, :]
            else:
                acc2[...] = total

            def f(step):
                to = refs["send2"].at[step - 1]
                to[...] = acc2[place.chunk(axes[2], step)].astype(BF16)
                return to, refs["recv2"].at[step - 1]

            to_each("rs", 2, f)

        def end_2():
            wait_all(recv_sem, "rs", 2)
            mine = refs["acc2"][place.chunk(axes[2], 0)]
            update(lax.fori_loop(0, self.counts[2], lambda n, t: t + refs["recv2"][n].astype(F32), mine))
            if layer == 1:
                for d, k in self.ring:
                    if k < self.far[d]:
                        wait(send_sem, "rs", 0, self.ring.index((d, k)))
                place.tell(free_sem.at[place_of])
            mine_copy(0).start()
            to_each("ag", 0, lambda step: (new.at[:, cols], part(0, 0)))

        def mine_copy(i):
            return pltpu.make_async_copy(new.at[:, cols] if i == 0 else refs["rows"].at[layer], part(i, 0), local_sem.at[first_local + 2 + 2 * layer + i])

        def next_back(i):
            wait_all(recv_sem, "ag", i - 1)
            if i == 1:
                mine_copy(0).wait()
            if self.kind == "down":
                if i == 1:
                    for z in range(8):
                        refs["flat"][22 * z : 22 * z + 22, :] = refs["blocks"][layer, z, :22, :].astype(F32)
                    refs["rows"][layer] = refs["flat"][...].astype(BF16)
                    mine_copy(1).start()
                else:
                    mine_copy(1).wait()
            if i == 1:
                to_each("ag", 1, lambda step: (refs["rows"].at[layer] if self.kind == "down" else part(1, 0), part(1, 0)))
            else:
                for d in (1, -1):
                    ring_back(d, 1)

        def forward(d, k):
            wait(recv_sem, "ag", 2, self.ring.index((d, k - 1)))
            ring_back(d, k)

        def finish():
            for d in (1, -1):
                wait(recv_sem, "ag", 2, self.ring.index((d, self.far[d])))
            for i in range(3):
                wait_all(send_sem, "ag", i)
                if layer == 0:
                    wait_all(send_sem, "rs", i)

        def listed(what, i, ms):
            axis = (axes if what == "rs" else back)[i]
            held = 8
            for a in back[:i]:
                held *= SIZE[a]
            nbytes = volume(shapes[i]) if what == "rs" else 2 * self.width * ((24, 176, 704)[i] if self.kind == "down" else held)
            n, found = SIZE[axis], []
            for d, k in ms:
                hops = 1 if d else min(k, n - k)
                way = d or (1 if 2 * k < n or 2 * k == n and self.role == 0 else -1)
                found.append((name(what, i, d, k), (axis, way), nbytes * hops, 0.7 * (hops - 1)))
            return found

        def all_of(what, i):
            return [(0, k) for k in range(1, self.counts[i if what == "rs" else 3 + i] + 1)]

        def names(what, i, ms):
            return [name(what, i, *m) for m in ms]

        far = self.far
        todo = [Action([], begin, listed("rs", 0, [(d, far[d]) for d in (1, -1)]), 0.2)]
        for k in range(max(far.values()) - 1, 0, -1):
            for d in (1, -1):
                if k < far[d]:
                    todo.append(Action([name("rs", 0, d, k + 1)], functools.partial(add, d, k), listed("rs", 0, [(d, k)]), 0.5))
        todo.append(Action(names("rs", 0, [(1, 1), (-1, 1)]), end_0, listed("rs", 1, all_of("rs", 1)), 0.7))
        todo.append(Action(names("rs", 1, all_of("rs", 1)), end_1, listed("rs", 2, all_of("rs", 2)), 0.4))
        todo.append(Action(names("rs", 2, all_of("rs", 2)), end_2, listed("ag", 0, all_of("ag", 0)), 0.6, True))
        todo.append(Action(names("ag", 0, all_of("ag", 0)), functools.partial(next_back, 1), listed("ag", 1, all_of("ag", 1)), 0.3))
        todo.append(Action(names("ag", 1, all_of("ag", 1)), functools.partial(next_back, 2), listed("ag", 2, [(1, 1), (-1, 1)]), 0.2))
        for k in range(2, max(far.values()) + 1):
            for d in (1, -1):
                if k <= far[d]:
                    todo.append(Action([name("ag", 2, d, k - 1)], functools.partial(forward, d, k), listed("ag", 2, [(d, k)]), 0.1))
        todo.append(Action(names("ag", 2, [(d, far[d]) for d in (1, -1)]), finish, [], 0.3))
        return todo


NN = (((1,), (0,)), ((), ()))
NT = (((1,), (1,)), ((), ()))
TN = (((0,), (0,)), ((), ()))
KINDS = ("gate", "up", "down")
ROWS = {"gate": 8, "up": 8, "down": 22}
VIEWS = {"gate": (4, 4, 8, 8, FF), "up": (4, 4, 8, 8, FF), "down": (4, 4, 176, D)}
TILE = 256
TILES = FF // TILE
HALF = T // 2


def dot(a, b, dims=NN):
    return lax.dot_general(a, b, dims, preferred_element_type=F32)


def params(mib=60):
    return pltpu.CompilerParams(vmem_limit_bytes=mib * 1024 * 1024)


def normed(h):
    wide = h.astype(F32)
    return (wide * lax.rsqrt(jnp.mean(wide * wide, -1, keepdims=True) + 1e-6)).astype(BF16)


def gates(x, w_gate, w_up, layer):
    def kernel(x_ref, wg, wu, a_ref, g_ref, u_ref, p_ref):
        @pl.when(pl.program_id(0) == 0)
        def _():
            a_ref[...] = normed(x_ref[...])

        a = a_ref[...]
        g, u = dot(a, wg[0]), dot(a, wu[0])
        g_ref[...], u_ref[...] = g, u
        p_ref[...] = (g * jax.nn.sigmoid(g) * u).astype(BF16)

    whole = pl.BlockSpec((T, D), lambda j: (0, 0))
    w = pl.BlockSpec((1, D, TILE), lambda j: (layer, 0, j))
    o = pl.BlockSpec((T, TILE), lambda j: (0, j))
    shapes = [((T, D), BF16), ((T, FF), F32), ((T, FF), F32), ((T, FF), BF16)]
    return pl.pallas_call(
        kernel,
        grid=(TILES,),
        in_specs=[whole, w, w],
        out_specs=[whole, o, o, o],
        out_shape=[jax.ShapeDtypeStruct(*s) for s in shapes],
        compiler_params=params(),
        name="gates",
    )(x, w_gate, w_up)


def down(p, w_down, h, layer, rows=512):
    def kernel(p_ref, w, h_ref, o_ref, a_ref):
        h1 = h_ref[...] + dot(p_ref[...], w[0]).astype(BF16)
        o_ref[...] = h1
        a_ref[...] = normed(h1)

    def row(n):
        return pl.BlockSpec((rows, n), lambda i: (i, 0))

    return pl.pallas_call(
        kernel,
        grid=(T // rows,),
        in_specs=[row(FF), pl.BlockSpec((1, FF, D), lambda i: (layer, 0, 0), pipeline_mode=pl.Buffered(1)), row(D)],
        out_specs=[row(D), row(D)],
        out_shape=[jax.ShapeDtypeStruct((T, D), BF16)] * 2,
        compiler_params=params(),
        name="down",
    )(p, w_down, h)


def split(g, u, dp):
    s = jax.nn.sigmoid(g)
    silu = g * s
    return silu * u, dp * u * (s + silu * (1 - s)), dp * silu


def tile(j):
    return pl.ds(pl.multiple_of(j * TILE, TILE), TILE)


LAST = (TILES, (4.0, 2.0, 1.3))
STATES = (8, (3.8,))
DOWN0 = (TILES, (1.9,))
FIRST = (TILES, (2.0, 2.3))
PARTS = (LAST, STATES, DOWN0, FIRST)


def tick_list():
    times, starts = [], []
    for n, each_time in PARTS:
        starts.append(len(times))
        times += list(each_time) * n
        times.append(0.5)
    return times, starts


STRIPS = [
    ("gate", 0, 768, 1, "zxy"),
    ("up", 0, 768, 0, "zxy"),
    ("gate", 768, 768, 1, "xyz"),
    ("up", 768, 768, 0, "yxz"),
    ("gate", 1536, 512, 1, "xyz"),
    ("up", 1536, 512, 1, "zxy"),
    ("gate", 2048, 512, 0, "zxy"),
    ("up", 2048, 512, 1, "yxz"),
    ("gate", 2560, 256, 0, "xyz"),
    ("up", 2560, 256, 1, "zxy"),
    ("down", 0, 256, 0, "xyz"),
    ("down", 256, 256, 1, "xyz"),
    ("down", 512, 256, 0, "yxz"),
    ("down", 768, 256, 0, "yxz"),
]


def releases(layer, strip, starts):
    last_tile = (strip.start + strip.width) // TILE - 1
    if layer == 1:
        n = len(LAST[1])
        return starts[0] + (TILES * n if strip.kind == "down" or last_tile == TILES - 1 else last_tile * n + n - 1)
    if strip.kind == "down":
        return starts[2] + TILES * len(DOWN0[1])
    n = len(FIRST[1])
    return starts[3] + (TILES * n if last_tile == TILES - 1 else (last_tile + 1) * n)


def make_strips():
    return [Strip(*s) for s in STRIPS]


def backward(a1, h1, dy, a0, p0, gate0, up0, weights, blocks, m, v):
    strips = make_strips()
    n_messages = MESSAGES * len(strips)
    scratch, names = [], []
    for s in strips:
        for k, shape in s.scratch().items():
            names.append((s, k))
            scratch.append(shape)

    def kernel(*refs):
        a1, h1, dy, a0, p0, gate0, up0, wg, wu, wd = refs[:10]
        old, m, v = (dict(zip(KINDS, refs[10 + 3 * i :])) for i in range(3))
        outs, sums = (dict(zip(KINDS, refs[19 + 3 * i :])) for i in range(2))
        grads = [dict(zip(KINDS, refs[25 + 3 * i :])) for i in range(2)]
        dgate, dup, dh = refs[31:34]
        refs = refs[34:]
        new = dict(zip(KINDS, refs))
        send_sem, recv_sem, local_sem, free_sem = refs[3:7]
        refs = refs[7:]
        place = Place()
        place.greet()
        new["down"][...] = jnp.zeros(new["down"].shape, BF16)
        times, starts = tick_list()
        chains, before = [], {}
        for n, s in enumerate(strips):
            mine = {k: r for (t, k), r in zip(names, refs) if t is s}
            for layer in (1, 0):

                def update(g, s=s, layer=layer):
                    rows = ROWS[s.kind]
                    at = (layer, pl.ds(0, rows), s.cols)
                    g = g[:rows].astype(BF16)
                    sums[s.kind][at] = g
                    g = g.astype(F32)
                    w = old[s.kind][at].astype(F32)
                    m1 = 0.9 * m[s.kind][at] + 0.1 * g
                    v1 = 0.95 * v[s.kind][at] + 0.05 * g * g
                    new[s.kind][at] = (w - 0.02 * (m1 * lax.rsqrt(v1 + 1e-8) + 0.1 * w)).astype(BF16)

                grad = grads[layer][s.kind].reshape(*VIEWS[s.kind])
                sems = (send_sem, recv_sem, local_sem, free_sem, n)
                a = s.chain(place, layer, grad, new[s.kind].at[layer], outs[s.kind].at[layer], mine, sems, update)
                chains.append(Chain(a, releases(layer, s, starts), before.get(s)))
                before[s] = chains[-1]
        placed, rest, _ = plan(chains, times)

        def tick(part, j, i):
            n, each_time = PARTS[part]
            per = len(each_time)
            if j is None:
                for a in placed[starts[part] + n * per]:
                    a.do()
                return
            for when in range(n):
                here = placed[starts[part] + when * per + i]
                if here:

                    @pl.when(j == when)
                    def _(here=here):
                        for a in here:
                            a.do()

        last_part(tick, a1, dy, wg.at[1], wu.at[1], wd.at[1], dgate, dup, grads[1])
        states_part(tick, dgate, dup, wg.at[1], wu.at[1], h1, dy, dh)
        down0_part(tick, p0, dh, grads[0])
        first_part(tick, a0, dh, wd.at[0], gate0, up0, grads[0])
        for a in rest:
            a.do()

    hbm = pl.BlockSpec(memory_space=pl.ANY)
    vmem = pl.BlockSpec(memory_space=pltpu.VMEM)
    wide = [jax.ShapeDtypeStruct((2, *VIEWS[k]), BF16) for k in KINDS]
    own = [jax.ShapeDtypeStruct((2, ROWS[k], VIEWS[k][-1]), BF16) for k in KINDS]
    local = [jax.ShapeDtypeStruct((FF, D) if k == "down" else (D, FF), BF16) for _ in range(2) for k in KINDS]
    local += [jax.ShapeDtypeStruct((T, FF), BF16)] * 2 + [jax.ShapeDtypeStruct((T, D), BF16)]
    out = pl.pallas_call(
        kernel,
        out_shape=wide + own + local,
        in_specs=[hbm] * 10 + [vmem] * 9,
        out_specs=[hbm] * 3 + [vmem] * 3 + [hbm] * 9,
        scratch_shapes=[pltpu.VMEM((2, -(-ROWS[k] // 8) * 8, VIEWS[k][-1]), BF16) for k in KINDS]
        + [pltpu.SemaphoreType.DMA((n_messages,))] * 2
        + [pltpu.SemaphoreType.DMA((6 * len(strips),)), pltpu.SemaphoreType.REGULAR((len(strips),))]
        + scratch,
        compiler_params=pltpu.CompilerParams(collective_id=1, has_side_effects=True, vmem_limit_bytes=67043328),
        name="backward",
    )(a1, h1, dy, a0, p0, gate0, up0, *weights, *blocks, *m, *v)
    return out[:3], out[3:6]


def last_part(tick, a1, dy, wg, wu, wd, dgate, dup, grads):
    def body(a, y, g_tile, u_tile, d_tile, p, dgu, og, ou, od, sem, in_sem, out_sem):
        dg, du = dgu.at[:, pl.ds(0, TILE)], dgu.at[:, pl.ds(TILE, TILE)]

        first = [pltpu.make_async_copy(s, d, sem.at[i]) for i, (s, d) in enumerate(((a1, a), (dy, y)))]

        def ins(j):
            s = lax.rem(j, 2)
            pairs = ((wg.at[:, tile(j)], g_tile.at[s]), (wu.at[:, tile(j)], u_tile.at[s]), (wd.at[tile(j)], d_tile.at[s]))
            return [pltpu.make_async_copy(src, dst, in_sem.at[s, i]) for i, (src, dst) in enumerate(pairs)]

        def outs(j):
            pairs = ((og, grads["gate"].at[:, tile(j)]), (ou, grads["up"].at[:, tile(j)]), (od, grads["down"].at[tile(j)]))
            pairs += ((dg, dgate.at[:, tile(j)]), (du, dup.at[:, tile(j)]))
            return [pltpu.make_async_copy(src, dst, out_sem.at[i]) for i, (src, dst) in enumerate(pairs)]

        for c in first + ins(jnp.int32(0)):
            c.start()
        for c in first:
            c.wait()

        def go(j, carry):
            s = lax.rem(j, 2)
            for c in ins(j):
                c.wait()

            @pl.when(j < TILES - 1)
            def _():
                for c in ins(j + 1):
                    c.start()

            for half in range(2):
                rows = pl.ds(half * HALF, HALF)
                g, u = dot(a[rows, :], g_tile[s]), dot(a[rows, :], u_tile[s])
                dp = dot(y[rows, :], d_tile[s], NT).astype(BF16).astype(F32)
                p_, dg_, du_ = split(g, u, dp)
                p[rows, :], dgu[rows, :TILE], dgu[rows, TILE:] = p_.astype(BF16), dg_.astype(BF16), du_.astype(BF16)
            o = outs(j)
            o[3].start()
            o[4].start()
            tick(0, j, 0)
            both = dot(a[...], dgu[...], TN).astype(BF16)
            og[...], ou[...] = both[:, :TILE], both[:, TILE:]
            o[0].start()
            o[1].start()
            tick(0, j, 1)

            @pl.when(j > 0)
            def _():
                outs(j - 1)[2].wait()

            od[...] = dot(p[...], y[...], TN).astype(BF16)
            o[2].start()
            for i in (3, 4, 0, 1):
                o[i].wait()
            tick(0, j, 2)
            return carry

        lax.fori_loop(0, TILES, go, 0)
        outs(jnp.int32(TILES - 1))[2].wait()
        tick(0, None, 0)

    tiles = [pltpu.VMEM((2, D, TILE), BF16)] * 2 + [pltpu.VMEM((2, TILE, D), BF16)]
    pl.run_scoped(
        body,
        *[pltpu.VMEM((T, D), BF16)] * 2,
        *tiles,
        pltpu.VMEM((T, TILE), BF16),
        pltpu.VMEM((T, 2 * TILE), BF16),
        *[pltpu.VMEM((D, TILE), BF16)] * 2,
        pltpu.VMEM((TILE, D), BF16),
        pltpu.SemaphoreType.DMA((2,)),
        pltpu.SemaphoreType.DMA((2, 3)),
        pltpu.SemaphoreType.DMA((5,)),
    )


def states_part(tick, dgate, dup, wg, wu, h1, dy, dh, rows=256):
    n = T // rows

    def body(wg_all, wu_all, dg, du, h, y, o, sem, in_sem, out_sem):
        first = [pltpu.make_async_copy(s, d, sem.at[i]) for i, (s, d) in enumerate(((wg, wg_all), (wu, wu_all)))]

        def at(j):
            return pl.ds(pl.multiple_of(j * rows, rows), rows)

        def ins(j):
            s = lax.rem(j, 2)
            pairs = ((dgate, dg), (dup, du), (h1, h), (dy, y))
            return [pltpu.make_async_copy(src.at[at(j)], dst.at[s], in_sem.at[s, i]) for i, (src, dst) in enumerate(pairs)]

        def out(j):
            return pltpu.make_async_copy(o, dh.at[at(j)], out_sem)

        for c in first + ins(jnp.int32(0)):
            c.start()
        for c in first:
            c.wait()

        def go(j, carry):
            s = lax.rem(j, 2)
            for c in ins(j):
                c.wait()

            @pl.when(j < n - 1)
            def _():
                for c in ins(j + 1):
                    c.start()

            da = (dot(dg[s], wg_all[...], NT) + dot(du[s], wu_all[...], NT)).astype(BF16).astype(F32)
            wide = h[s].astype(F32)
            scale = lax.rsqrt(jnp.mean(wide * wide, -1, keepdims=True) + 1e-6)
            inner = jnp.mean(da * wide, -1, keepdims=True)
            back = da * scale - wide * (scale * scale * scale * inner)

            @pl.when(j > 0)
            def _():
                out(j - 1).wait()

            o[...] = (y[s].astype(F32) + back).astype(BF16)
            out(j).start()
            tick(1, j, 0)
            return carry

        lax.fori_loop(0, n, go, 0)
        out(jnp.int32(n - 1)).wait()
        tick(1, None, 0)

    pl.run_scoped(
        body,
        *[pltpu.VMEM((D, FF), BF16)] * 2,
        *[pltpu.VMEM((2, rows, FF), BF16)] * 2,
        *[pltpu.VMEM((2, rows, D), BF16)] * 2,
        pltpu.VMEM((rows, D), BF16),
        pltpu.SemaphoreType.DMA((2,)),
        pltpu.SemaphoreType.DMA((2, 4)),
        pltpu.SemaphoreType.DMA,
    )


def down0_part(tick, p0, dh, grads):
    def body(y, p, od, sem, in_sem, out_sem):
        first = pltpu.make_async_copy(dh, y, sem)

        def load(j):
            s = lax.rem(j, 2)
            return pltpu.make_async_copy(p0.at[:, tile(j)], p.at[s], in_sem.at[s])

        def out(j):
            return pltpu.make_async_copy(od, grads["down"].at[tile(j)], out_sem)

        first.start()
        load(jnp.int32(0)).start()
        first.wait()

        def go(j, carry):
            s = lax.rem(j, 2)
            load(j).wait()

            @pl.when(j < TILES - 1)
            def _():
                load(j + 1).start()

            @pl.when(j > 0)
            def _():
                out(j - 1).wait()

            od[...] = dot(p[s], y[...], TN).astype(BF16)
            out(j).start()
            tick(2, j, 0)
            return carry

        lax.fori_loop(0, TILES, go, 0)
        out(jnp.int32(TILES - 1)).wait()
        tick(2, None, 0)

    pl.run_scoped(
        body,
        pltpu.VMEM((T, D), BF16),
        pltpu.VMEM((2, T, TILE), BF16),
        pltpu.VMEM((TILE, D), BF16),
        pltpu.SemaphoreType.DMA,
        pltpu.SemaphoreType.DMA((2,)),
        pltpu.SemaphoreType.DMA,
    )


def first_part(tick, a0, dh, wd, gate0, up0, grads):
    def body(a, y, d_tile, g, u, dgu, og, ou, sem, in_sem, out_sem):
        first = [pltpu.make_async_copy(s, d, sem.at[i]) for i, (s, d) in enumerate(((a0, a), (dh, y)))]

        def ins(j):
            s = lax.rem(j, 2)
            pairs = ((wd.at[tile(j)], d_tile.at[s]), (gate0.at[:, tile(j)], g.at[s]), (up0.at[:, tile(j)], u.at[s]))
            return [pltpu.make_async_copy(src, dst, in_sem.at[s, i]) for i, (src, dst) in enumerate(pairs)]

        def outs(j):
            pairs = ((og, grads["gate"].at[:, tile(j)]), (ou, grads["up"].at[:, tile(j)]))
            return [pltpu.make_async_copy(src, dst, out_sem.at[i]) for i, (src, dst) in enumerate(pairs)]

        for c in first + ins(jnp.int32(0)):
            c.start()
        for c in first:
            c.wait()

        def go(j, carry):
            s = lax.rem(j, 2)
            for c in ins(j):
                c.wait()

            @pl.when(j < TILES - 1)
            def _():
                for c in ins(j + 1):
                    c.start()

            for half in range(2):
                rows = pl.ds(half * HALF, HALF)
                dp = dot(y[rows, :], d_tile[s], NT).astype(BF16).astype(F32)
                _, dg_, du_ = split(g[s, rows, :], u[s, rows, :], dp)
                dgu[rows, :TILE], dgu[rows, TILE:] = dg_.astype(BF16), du_.astype(BF16)

            @pl.when(j > 0)
            def _():
                for c in outs(j - 1):
                    c.wait()

            tick(3, j, 0)
            both = dot(a[...], dgu[...], TN).astype(BF16)
            og[...], ou[...] = both[:, :TILE], both[:, TILE:]
            for c in outs(j):
                c.start()
            tick(3, j, 1)
            return carry

        lax.fori_loop(0, TILES, go, 0)
        for c in outs(jnp.int32(TILES - 1)):
            c.wait()
        tick(3, None, 0)

    pl.run_scoped(
        body,
        *[pltpu.VMEM((T, D), BF16)] * 2,
        pltpu.VMEM((2, TILE, D), BF16),
        *[pltpu.VMEM((2, T, TILE), F32)] * 2,
        pltpu.VMEM((T, 2 * TILE), BF16),
        *[pltpu.VMEM((D, TILE), BF16)] * 2,
        pltpu.SemaphoreType.DMA((2,)),
        pltpu.SemaphoreType.DMA((2, 3)),
        pltpu.SemaphoreType.DMA((2,)),
    )


def moments(sums, m, v):
    def kernel(*refs):
        for g, m_ref, v_ref, new_m, new_v in zip(*(refs[3 * i :][:3] for i in range(5))):
            grad = g[...].astype(F32)
            new_m[...] = 0.9 * m_ref[...] + 0.1 * grad
            new_v[...] = 0.95 * v_ref[...] + 0.05 * grad * grad

    shapes = [jax.ShapeDtypeStruct(t.shape, F32) for t in (*m, *v)]
    out = pl.pallas_call(kernel, out_shape=shapes, name="moments")(*sums, *m, *v)
    return out[:3], out[3:]


def step(x, dy, *arrays):
    weights, m, v = (arrays[i : i + 3] for i in (0, 3, 6))
    w_gate, w_up, w_down = weights
    x, dy = x[0], dy[0]
    me = lax.axis_index("dp")
    blocks = [lax.dynamic_slice_in_dim(w, me * ROWS[k], ROWS[k], 1) for k, w in zip(KINDS, weights)]
    a0, gate0, up0, p0 = gates(x, w_gate, w_up, 0)
    h1, a1 = down(p0, w_down, x, 0)
    whole, sums = backward(a1, h1, dy, a0, p0, gate0, up0, weights, blocks, m, v)
    new_m, new_v = moments(sums, m, v)
    return (*(t.reshape(2, -1, t.shape[-1]) for t in whole), *new_m, *new_v)


def solution(mesh):
    P = jax.sharding.PartitionSpec
    data, state = P(("rep", "dp")), P(None, "dp")
    return jax.shard_map(
        step,
        mesh=mesh,
        in_specs=(data, data, P(), P(), P(), *[state] * 6),
        out_specs=(*[P("rep")] * 3, *[P("rep", "dp")] * 6),
        check_vma=False,
    )
```

```python
import functools

import jax
import jax.numpy as jnp
from jax import lax
from jax.experimental import pallas as pl
from jax.experimental.pallas import tpu as pltpu

LOGICAL = pl.DeviceIdType.LOGICAL
F32, BF16 = jnp.float32, jnp.bfloat16
T, D, FF = 2048, 1024, 2816
SIZE = {"x": 4, "y": 4, "z": 8}
STRIDE = {"x": 32, "y": 8, "z": 1}
PARTNERS = 13
MESSAGES = 39


class Place:
    def __init__(self):
        me = self.me = lax.axis_index("dp")
        self.at = {"x": me // 32, "y": (me // 8) % 4, "z": me % 8}
        self.number = lax.axis_index("rep") * 128 + me
        self.ring = {(axis, step): (self.at_step(axis, step), self.partner(axis, step)) for axis in "xyz" for step in (1, -1)}

    def at_step(self, axis, step):
        return lax.rem(self.at[axis] + (step + SIZE[axis] if isinstance(step, int) else step), SIZE[axis])

    def chunk(self, axis, step):
        return self.at[axis] if isinstance(step, int) and step == 0 else self.at_step(axis, step)

    def partner(self, axis, step):
        return self.number + (self.at_step(axis, step) - self.at[axis]) * STRIDE[axis]

    def tell(self, semaphore):
        for axis, n in SIZE.items():

            def one(step, c, axis=axis):
                pl.semaphore_signal(semaphore, inc=1, device_id=self.partner(axis, step), device_id_type=LOGICAL)
                return c

            lax.fori_loop(1, n, one, 0)

    def greet(self):
        barrier = pltpu.get_barrier_semaphore()
        self.tell(barrier)
        pl.semaphore_wait(barrier, PARTNERS)


class Action:
    def __init__(self, waits, do, sends, cost=0.3, frees=False):
        self.waits, self.do, self.sends, self.cost, self.frees = waits, do, sends, cost, frees


class Chain:
    def __init__(self, actions, release, before=None):
        self.actions, self.release, self.before, self.done, self.freed = actions, release, before, 0, None

    def ended(self):
        return self.done == len(self.actions)


RATE = 45.5e3


LATENCY = 3.0


def plan(chains, ticks, latency=LATENCY):
    free, arrive, now, placed, rest = {}, {}, 0.0, [], []

    def run(c, a, at):
        if a.frees:
            c.freed = at
        for name, link, nbytes, further in a.sends:
            begin = max(free.get(link, 0.0), at + a.cost)
            free[link] = begin + nbytes / RATE
            arrive[name] = free[link] + latency + further

    def ready(c, tick):
        if c.ended() or c.release > tick or (c.before and c.before.freed is None):
            return None
        waits = c.actions[c.done].waits
        known = [arrive[w] for w in waits if w in arrive] + [c.before.freed + latency if c.before else 0.0]
        return max(known) if len(known) > len(waits) else None

    for tick, time in enumerate(ticks):
        now += time
        here = []
        while True:
            best = min(((r, i) for i, c in enumerate(chains) if (r := ready(c, tick)) is not None and r <= now), default=None)
            if best is None:
                break
            c = chains[best[1]]
            a = c.actions[c.done]
            c.done += 1
            run(c, a, now)
            now += a.cost
            here.append(a)
        placed.append(here)
    while not all(c.ended() for c in chains):
        r, i = min((max(r, now), i) for i, c in enumerate(chains) if (r := ready(c, len(ticks))) is not None)
        c = chains[i]
        a = c.actions[c.done]
        c.done += 1
        now = max(r, now)
        run(c, a, now)
        now += a.cost
        rest.append(a)
    return placed, rest, now


def volume(shape):
    n = 2
    for v in shape:
        n *= v
    return n


def each(shape, f):
    if len(shape) > 3 or shape[-2] == 176 and len(shape) == 3:
        lax.fori_loop(0, shape[0], lambda i, c: (f((i,)), c)[1], 0)
    else:
        f((slice(None),) * len(shape))


class Strip:
    def __init__(self, kind, start, width, role, axes):
        self.kind, self.start, self.width, self.role, self.axes = kind, start, width, role, axes
        self.cols = pl.ds(start, width)
        left = [a for a in "xyz" if a != axes[0]]
        if kind == "down":
            shapes = ((4, 176), (176,), (24,))
        else:
            shapes = ((SIZE[left[0]], SIZE[left[1]], 8), (SIZE[left[1]], 8), (8,))
        self.shapes = [(*s, width) for s in shapes]
        self.back = axes[::-1]
        n = SIZE[axes[0]]
        self.far = {1: n // 2 if role == 0 else n // 2 - 1, -1: n // 2 if role == 1 else n // 2 - 1}
        self.ring = [(d, k) for d in (1, -1) for k in range(self.far[d], 0, -1)]
        self.counts = [SIZE[a] - 1 for a in (*axes, *self.back)]
        sums = {d: [d * k for k in range(self.far[d] - 1, 0, -1)] for d in (1, -1)}
        short = -1 if role == 0 else 1
        sums[short] = sums[short] + [0]
        self.own = [sums[-short] + sums[short]] if n == 4 else [sums[1], sums[-1]]

    def offset(self, layer, what, i):
        if what == "rs":
            return sum(self.counts[:i])
        return sum(self.counts[: 3 + i]) + layer * sum(self.counts[3:])

    def scratch(self):
        s = {"own": pltpu.VMEM((len(self.own), *self.shapes[0]), BF16), "acc1": pltpu.VMEM(self.shapes[1], F32)}
        s["acc2"] = pltpu.VMEM((SIZE[self.axes[2]], *self.shapes[2]), F32)
        for i in range(3):
            s[f"recv{i}"] = pltpu.VMEM((self.counts[i], *self.shapes[i]), BF16)
        for i in (1, 2):
            s[f"send{i}"] = pltpu.VMEM((self.counts[i], *self.shapes[i]), BF16)
        if self.kind == "down":
            s["flat"] = pltpu.VMEM(self.shapes[1], F32)
            s["blocks"] = pltpu.VMEM((2, 8, *self.shapes[2]), BF16)
            s["rows"] = pltpu.VMEM((2, *self.shapes[1]), BF16)
        return s

    def chain(self, place, layer, grad, new, out, refs, sems, update):
        send_sem, recv_sem, local_sem, free_sem, place_of = sems
        axes, back, shapes, cols = self.axes, self.back, self.shapes, self.cols
        base, first_local = place_of * MESSAGES, place_of * 6

        def name(*m):
            return (layer, id(self), *m)

        def raw(step):
            c = place.chunk(axes[0], step)
            if self.kind == "down":
                return grad.at[c, :, :, cols] if axes[0] == "x" else grad.at[:, c, :, cols]
            return grad.at[(*(c if a == axes[0] else slice(None) for a in "xyz"), slice(None), cols)]

        def received(d, k):
            return refs["recv0"].at[self.ring.index((d, k))]

        def source(d, k):
            return received(d, k + 1) if k < self.far[d] else raw(d * k)

        def part(i, step):
            c = place.chunk(back[i], step)
            if self.kind == "down" and i == 0:
                return refs["blocks"].at[layer, c]
            known = {a: (slice(None) if a in back[:i] else c if a == back[i] else place.chunk(a, 0)) for a in "xyz"}
            if self.kind == "down":
                return out.at[known["x"], known["y"], :, cols]
            return out.at[known["x"], known["y"], known["z"], :, cols]

        def like(what, i):
            return refs[f"recv{i}"].at[0] if what == "rs" else part(i, 0)

        def send(what, i, n, src, dst, device):
            n = base + self.offset(layer, what, i) + n
            pltpu.make_async_remote_copy(src, dst, send_sem.at[n], recv_sem.at[n], device_id=device, device_id_type=LOGICAL).start()

        def wait(sem, what, i, n):
            ref = like(what, i)
            pltpu.make_async_copy(ref, ref, sem.at[base + self.offset(layer, what, i) + n]).wait()

        def wait_all(sem, what, i):
            count = self.counts[i if what == "rs" else 3 + i]
            lax.fori_loop(0, count, lambda n, c: (wait(sem, what, i, n), c)[1], 0)

        def ring_send(d, k):
            send("rs", 0, self.ring.index((d, k)), source(d, k), received(d, k), place.ring[axes[0], d][1])

        def ring_back(d, k):
            there = part(2, -d * (k - 1))
            send("ag", 2, self.ring.index((d, k)), there, there, place.ring[back[2], d][1])

        def to_each(what, i, f):
            axis = (axes if what == "rs" else back)[i]

            def one(step, c):
                send(what, i, step - 1, *f(step), place.partner(axis, step))
                return c

            lax.fori_loop(1, SIZE[axis], one, 0)

        def own_copy(step):
            b = next(b for b, seq in enumerate(self.own) if step in seq)
            return pltpu.make_async_copy(raw(step), refs["own"].at[b], local_sem.at[first_local + b])

        def own(step):
            b = next(b for b, seq in enumerate(self.own) if step in seq)
            mine = refs["own"].at[b]
            pltpu.make_async_copy(mine, mine, local_sem.at[first_local + b]).wait()
            return mine

        def begin():
            if layer == 0:
                for i in (1, 2):
                    wait_all(send_sem, "rs", i)
                for d in (1, -1):
                    wait(send_sem, "rs", 0, self.ring.index((d, self.far[d])))
                pl.semaphore_wait(free_sem.at[place_of], PARTNERS)
            for d in (1, -1):
                ring_send(d, self.far[d])
            for seq in self.own:
                own_copy(seq[0]).start()

        def add(d, k):
            wait(recv_sem, "rs", 0, self.ring.index((d, k + 1)))
            theirs, mine = received(d, k + 1), own(d * k)

            def f(at):
                theirs[at] = (mine[at].astype(F32) + theirs[at].astype(F32)).astype(BF16)

            each(shapes[0], f)
            for seq in self.own:
                if d * k in seq[:-1]:
                    own_copy(seq[seq.index(d * k) + 1]).start()
            ring_send(d, k)

        def end_0():
            mine = own(0)
            for d in (1, -1):
                wait(recv_sem, "rs", 0, self.ring.index((d, 1)))

            def total(step):
                c = place.chunk(axes[1], step)
                return mine[c].astype(F32) + received(1, 1)[c].astype(F32) + received(-1, 1)[c].astype(F32)

            def f(step):
                to = refs["send1"].at[step - 1]
                to[...] = total(step).astype(BF16)
                return to, refs["recv1"].at[step - 1]

            to_each("rs", 1, f)
            refs["acc1"][...] = total(0)

        def end_1():
            wait_all(recv_sem, "rs", 1)
            acc2 = refs["acc2"]
            total = refs["acc1"][...]
            for n in range(self.counts[1]):
                total = total + refs["recv1"][n].astype(F32)
            if self.kind == "down":
                refs["flat"][...] = total
                for z in range(8):
                    acc2[z, :22, :] = refs["flat"][22 * z : 22 * z + 22, :]
            else:
                acc2[...] = total

            def f(step):
                to = refs["send2"].at[step - 1]
                to[...] = acc2[place.chunk(axes[2], step)].astype(BF16)
                return to, refs["recv2"].at[step - 1]

            to_each("rs", 2, f)

        def end_2():
            wait_all(recv_sem, "rs", 2)
            mine = refs["acc2"][place.chunk(axes[2], 0)]
            update(lax.fori_loop(0, self.counts[2], lambda n, t: t + refs["recv2"][n].astype(F32), mine))
            if layer == 1:
                for d, k in self.ring:
                    if k < self.far[d]:
                        wait(send_sem, "rs", 0, self.ring.index((d, k)))
                place.tell(free_sem.at[place_of])
            mine_copy(0).start()
            to_each("ag", 0, lambda step: (new.at[:, cols], part(0, 0)))

        def mine_copy(i):
            return pltpu.make_async_copy(new.at[:, cols] if i == 0 else refs["rows"].at[layer], part(i, 0), local_sem.at[first_local + 2 + 2 * layer + i])

        def next_back(i):
            wait_all(recv_sem, "ag", i - 1)
            if i == 1:
                mine_copy(0).wait()
            if self.kind == "down":
                if i == 1:
                    for z in range(8):
                        refs["flat"][22 * z : 22 * z + 22, :] = refs["blocks"][layer, z, :22, :].astype(F32)
                    refs["rows"][layer] = refs["flat"][...].astype(BF16)
                    mine_copy(1).start()
                else:
                    mine_copy(1).wait()
            if i == 1:
                to_each("ag", 1, lambda step: (refs["rows"].at[layer] if self.kind == "down" else part(1, 0), part(1, 0)))
            else:
                for d in (1, -1):
                    ring_back(d, 1)

        def forward(d, k):
            wait(recv_sem, "ag", 2, self.ring.index((d, k - 1)))
            ring_back(d, k)

        def finish():
            for d in (1, -1):
                wait(recv_sem, "ag", 2, self.ring.index((d, self.far[d])))
            for i in range(3):
                wait_all(send_sem, "ag", i)
                if layer == 0:
                    wait_all(send_sem, "rs", i)

        def listed(what, i, ms):
            axis = (axes if what == "rs" else back)[i]
            held = 8
            for a in back[:i]:
                held *= SIZE[a]
            nbytes = volume(shapes[i]) if what == "rs" else 2 * self.width * ((24, 176, 704)[i] if self.kind == "down" else held)
            n, found = SIZE[axis], []
            for d, k in ms:
                hops = 1 if d else min(k, n - k)
                way = d or (1 if 2 * k < n or 2 * k == n and self.role == 0 else -1)
                found.append((name(what, i, d, k), (axis, way), nbytes * hops, 0.7 * (hops - 1)))
            return found

        def all_of(what, i):
            return [(0, k) for k in range(1, self.counts[i if what == "rs" else 3 + i] + 1)]

        def names(what, i, ms):
            return [name(what, i, *m) for m in ms]

        far = self.far
        todo = [Action([], begin, listed("rs", 0, [(d, far[d]) for d in (1, -1)]), 0.06)]
        for k in range(max(far.values()) - 1, 0, -1):
            for d in (1, -1):
                if k < far[d]:
                    todo.append(Action([name("rs", 0, d, k + 1)], functools.partial(add, d, k), listed("rs", 0, [(d, k)]), 0.3 if SIZE[axes[0]] == 4 else 0.13))
        todo.append(Action(names("rs", 0, [(1, 1), (-1, 1)]), end_0, listed("rs", 1, all_of("rs", 1)), 0.4))
        todo.append(Action(names("rs", 1, all_of("rs", 1)), end_1, listed("rs", 2, all_of("rs", 2)), 0.35))
        todo.append(Action(names("rs", 2, all_of("rs", 2)), end_2, listed("ag", 0, all_of("ag", 0)), 0.5, True))
        todo.append(Action(names("ag", 0, all_of("ag", 0)), functools.partial(next_back, 1), listed("ag", 1, all_of("ag", 1)), 0.25))
        todo.append(Action(names("ag", 1, all_of("ag", 1)), functools.partial(next_back, 2), listed("ag", 2, [(1, 1), (-1, 1)]), 0.15))
        for k in range(2, max(far.values()) + 1):
            for d in (1, -1):
                if k <= far[d]:
                    todo.append(Action([name("ag", 2, d, k - 1)], functools.partial(forward, d, k), listed("ag", 2, [(d, k)]), 0.1))
        todo.append(Action(names("ag", 2, [(d, far[d]) for d in (1, -1)]), finish, [], 0.15))
        return todo


NN = (((1,), (0,)), ((), ()))
NT = (((1,), (1,)), ((), ()))
TN = (((0,), (0,)), ((), ()))
KINDS = ("gate", "up", "down")
ROWS = {"gate": 8, "up": 8, "down": 22}
VIEWS = {"gate": (4, 4, 8, 8, FF), "up": (4, 4, 8, 8, FF), "down": (4, 4, 176, D)}
TILE = 256
TILES = FF // TILE
HALF = T // 2


def dot(a, b, dims=NN):
    return lax.dot_general(a, b, dims, preferred_element_type=F32)


def normed(h):
    wide = h.astype(F32)
    return (wide * lax.rsqrt(jnp.mean(wide * wide, -1, keepdims=True) + 1e-6)).astype(BF16)


def split(g, u, dp):
    s = jax.nn.sigmoid(g)
    silu = g * s
    return silu * u, dp * u * (s + silu * (1 - s)), dp * silu


def tile(j):
    return pl.ds(pl.multiple_of(j * TILE, TILE), TILE)


LAST = (TILES, (4.1, 2.05, 1.4))
STATES = (8, (4.3,))
DOWN0 = (TILES, (1.76,))
FIRST = (TILES, (2.24, 2.4))
PARTS = (LAST, STATES, DOWN0, FIRST)


def tick_list():
    times, starts = [], []
    for n, each_time in PARTS:
        starts.append(len(times))
        times += list(each_time) * n
        times.append(0.5)
    return times, starts


STRIPS = [
    ("gate", 0, 768, 1, "zxy"),
    ("up", 0, 768, 0, "zxy"),
    ("gate", 768, 768, 0, "xyz"),
    ("up", 768, 768, 0, "yxz"),
    ("gate", 1536, 512, 1, "xyz"),
    ("up", 1536, 512, 0, "yxz"),
    ("gate", 2048, 512, 1, "zxy"),
    ("up", 2048, 512, 0, "yxz"),
    ("gate", 2560, 256, 0, "zxy"),
    ("up", 2560, 256, 1, "zxy"),
    ("down", 0, 256, 1, "yxz"),
    ("down", 256, 256, 1, "yxz"),
    ("down", 512, 256, 1, "xyz"),
    ("down", 768, 256, 0, "xyz"),
]


def releases(layer, strip, starts):
    last_tile = (strip.start + strip.width) // TILE - 1
    if layer == 1:
        n = len(LAST[1])
        return starts[0] + (TILES * n if strip.kind == "down" or last_tile == TILES - 1 else last_tile * n + n - 1)
    if strip.kind == "down":
        return starts[2] + TILES * len(DOWN0[1])
    n = len(FIRST[1])
    return starts[3] + (TILES * n if last_tile == TILES - 1 else (last_tile + 1) * n)


def make_strips():
    return [Strip(*s) for s in STRIPS]


def train(x, dy, weights, block, m, v):
    strips = make_strips()
    n_messages = MESSAGES * len(strips)
    scratch, names = [], []
    for s in strips:
        for k, shape in s.scratch().items():
            names.append((s, k))
            scratch.append(shape)

    def kernel(*refs):
        x, dy, wg, wu, wd = refs[:5]
        m, v = (dict(zip(KINDS, refs[6 + 3 * i :])) for i in range(2))
        outs, sums = (dict(zip(KINDS, refs[12 + 3 * i :])) for i in range(2))
        grads = [dict(zip(KINDS, refs[18 + 3 * i :])) for i in range(2)]
        dgate, dup, p0, gate0, up0, a0, h1 = refs[24:31]
        old = {"gate": refs[31], "up": refs[32], "down": refs[5]}
        refs = refs[33:]
        new = dict(zip(KINDS, refs))
        send_sem, recv_sem, local_sem, free_sem, old_sem = refs[3:8]
        refs = refs[8:]
        place = Place()
        mine = pl.ds(pl.multiple_of(place.me * 8, 8), 8)
        loads = [pltpu.make_async_copy(w.at[:, mine], old[k], old_sem.at[i]) for i, (k, w) in enumerate((("gate", wg), ("up", wu)))]
        for c in loads:
            c.start()
        barrier = pltpu.get_barrier_semaphore()
        place.tell(barrier)
        for c in loads:
            c.wait()
        new["down"][...] = jnp.zeros(new["down"].shape, BF16)
        times, starts = tick_list()
        chains, before = [], {}
        for n, s in enumerate(strips):
            mine = {k: r for (t, k), r in zip(names, refs) if t is s}
            for layer in (1, 0):

                def update(g, s=s, layer=layer):
                    rows = ROWS[s.kind]
                    at = (layer, pl.ds(0, rows), s.cols)
                    g = g[:rows].astype(BF16)
                    sums[s.kind][at] = g
                    g = g.astype(F32)
                    w = old[s.kind][at].astype(F32)
                    moments_at = (at[1], layer, s.cols) if s.kind == "down" else at
                    m1 = 0.9 * m[s.kind][moments_at] + 0.1 * g
                    v1 = 0.95 * v[s.kind][moments_at] + 0.05 * g * g
                    new[s.kind][at] = (w - 0.02 * (m1 * lax.rsqrt(v1 + 1e-8) + 0.1 * w)).astype(BF16)

                grad = grads[layer][s.kind].reshape(*VIEWS[s.kind])
                sems = (send_sem, recv_sem, local_sem, free_sem, n)
                a = s.chain(place, layer, grad, new[s.kind].at[layer], outs[s.kind].at[layer], mine, sems, update)
                chains.append(Chain(a, releases(layer, s, starts), before.get(s)))
                before[s] = chains[-1]
        placed, rest, _ = plan(chains, times)

        def tick(part, j, i):
            n, each_time = PARTS[part]
            per = len(each_time)
            if j is None:
                for a in placed[starts[part] + n * per]:
                    a.do()
                return
            for when in range(n):
                here = placed[starts[part] + when * per + i]
                if here:

                    @pl.when(j == when)
                    def _(here=here):
                        for a in here:
                            a.do()

        def parts(a, y, sem):
            load = pltpu.make_async_copy(dy, y, sem)
            load.start()
            forward_part(x, wg.at[0], wu.at[0], wd.at[0], a0, gate0, up0, p0, h1, a)
            load.wait()
            pl.semaphore_wait(barrier, PARTNERS)
            last_part(tick, a, y, wg.at[1], wu.at[1], wd.at[1], dgate, dup, grads[1])
            states_part(tick, dgate, dup, wg.at[1], wu.at[1], h1, y, a)
            load = pltpu.make_async_copy(a0, a, sem)
            load.start()
            down0_part(tick, p0, y, grads[0])
            load.wait()
            first_part(tick, a, y, wd.at[0], gate0, up0, grads[0])

        pl.run_scoped(parts, *[pltpu.VMEM((T, D), BF16)] * 2, pltpu.SemaphoreType.DMA)
        for a in rest:
            a.do()

    hbm = pl.BlockSpec(memory_space=pl.ANY)
    vmem = pl.BlockSpec(memory_space=pltpu.VMEM)
    wide = [jax.ShapeDtypeStruct((2, *VIEWS[k]), BF16) for k in KINDS]
    own = [jax.ShapeDtypeStruct((2, ROWS[k], VIEWS[k][-1]), BF16) for k in KINDS]
    local = [jax.ShapeDtypeStruct((FF, D) if k == "down" else (D, FF), BF16) for _ in range(2) for k in KINDS]
    local += [jax.ShapeDtypeStruct((T, FF), t) for t in (BF16, BF16, BF16, F32, F32)] + [jax.ShapeDtypeStruct((T, D), BF16)] * 2
    out = pl.pallas_call(
        kernel,
        out_shape=wide + own + local,
        in_specs=[hbm] * 5 + [vmem] * 7,
        out_specs=[hbm] * 3 + [vmem] * 3 + [hbm] * 13,
        scratch_shapes=[pltpu.VMEM((2, 8, FF), BF16)] * 2
        + [pltpu.VMEM((2, -(-ROWS[k] // 8) * 8, VIEWS[k][-1]), BF16) for k in KINDS]
        + [pltpu.SemaphoreType.DMA((n_messages,))] * 2
        + [pltpu.SemaphoreType.DMA((6 * len(strips),)), pltpu.SemaphoreType.REGULAR((len(strips),)), pltpu.SemaphoreType.DMA((2,))]
        + scratch,
        compiler_params=pltpu.CompilerParams(collective_id=1, has_side_effects=True, vmem_limit_bytes=67043328),
        name="train",
    )(x, dy, *weights, block, *m, *v)
    return out[:3], out[3:6]


def forward_part(x, wg, wu, wd, a0, gate0, up0, p0, h1, a):
    rows, tall = 256, 512
    n, n_tall = T // rows, T // tall

    def at(j, rows=rows):
        return pl.ds(pl.multiple_of(j * rows, rows), rows)

    def body(g_tile, u_tile, in_sem, a_sem):
        store_a = pltpu.make_async_copy(a, a0, a_sem)

        def ins(j):
            s = lax.rem(j, 2)
            pairs = ((wg, g_tile), (wu, u_tile))
            return [pltpu.make_async_copy(src.at[:, tile(j)], dst.at[s], in_sem.at[s, i]) for i, (src, dst) in enumerate(pairs)]

        def norm(h, sem):
            def load(j):
                return pltpu.make_async_copy(x.at[at(j)], h.at[at(j)], sem.at[j])

            lax.fori_loop(0, n, lambda j, c: (load(j).start(), c)[1], 0)
            for c in ins(jnp.int32(0)):
                c.start()

            def go(j, carry):
                load(j).wait()
                a[at(j), :] = normed(h[at(j), :])
                return carry

            lax.fori_loop(0, n, go, 0)

        def gates(g, u, p, out_sem):
            def outs(j):
                s = lax.rem(j, 2)
                pairs = ((g, gate0), (u, up0), (p, p0))
                return [pltpu.make_async_copy(src.at[s], dst.at[:, tile(j)], out_sem.at[s, i]) for i, (src, dst) in enumerate(pairs)]

            def go(j, carry):
                s = lax.rem(j, 2)
                for c in ins(j):
                    c.wait()

                @pl.when(j < TILES - 1)
                def _():
                    for c in ins(j + 1):
                        c.start()

                @pl.when(j > 1)
                def _():
                    for c in outs(j - 2):
                        c.wait()

                for half in range(2):
                    rows = pl.ds(half * HALF, HALF)
                    gate, up = dot(a[rows, :], g_tile[s]), dot(a[rows, :], u_tile[s])
                    g[s, rows, :], u[s, rows, :] = gate, up
                    p[s, rows, :] = (gate * jax.nn.sigmoid(gate) * up).astype(BF16)
                for c in outs(j):
                    c.start()
                return carry

            lax.fori_loop(0, TILES, go, 0)
            for j in (TILES - 2, TILES - 1):
                for c in outs(jnp.int32(j)):
                    c.wait()

        def next_states(w, p, h, o, w_sem, sem, out_sem):
            load_w = pltpu.make_async_copy(wd, w, w_sem)
            def loads(j):
                s = lax.rem(j, 2)
                return [pltpu.make_async_copy(src.at[at(j, tall)], dst.at[s], sem.at[s, i]) for i, (src, dst) in enumerate(((p0, p), (x, h)))]

            def out(j):
                s = lax.rem(j, 2)
                return pltpu.make_async_copy(o.at[s], h1.at[at(j, tall)], out_sem.at[s])

            for c in (load_w, *loads(jnp.int32(0))):
                c.start()
            store_a.wait()
            load_w.wait()

            def go(j, carry):
                s = lax.rem(j, 2)
                for c in loads(j):
                    c.wait()

                @pl.when(j < n_tall - 1)
                def _():
                    for c in loads(j + 1):
                        c.start()

                @pl.when(j > 1)
                def _():
                    out(j - 2).wait()

                a[at(lax.max(j - 1, 0), tall), :] = normed(o[1 - s])
                o[s] = h[s] + dot(p[s], w[...]).astype(BF16)
                out(j).start()
                return carry

            o[1] = jnp.zeros((tall, D), BF16)
            lax.fori_loop(0, n_tall, go, 0)
            a[at(n_tall - 1, tall), :] = normed(o[(n_tall - 1) % 2])
            for j in (n_tall - 2, n_tall - 1):
                out(jnp.int32(j)).wait()

        pl.run_scoped(norm, pltpu.VMEM((T, D), BF16), pltpu.SemaphoreType.DMA((n,)))
        store_a.start()
        stores = [pltpu.VMEM((2, T, TILE), t) for t in (F32, F32, BF16)]
        pl.run_scoped(gates, *stores, pltpu.SemaphoreType.DMA((2, 3)))
        tiles = [pltpu.VMEM((FF, D), BF16), pltpu.VMEM((2, tall, FF), BF16), pltpu.VMEM((2, tall, D), BF16), pltpu.VMEM((2, tall, D), BF16)]
        pl.run_scoped(next_states, *tiles, pltpu.SemaphoreType.DMA, pltpu.SemaphoreType.DMA((2, 2)), pltpu.SemaphoreType.DMA((2,)))

    pl.run_scoped(
        body,
        *[pltpu.VMEM((2, D, TILE), BF16)] * 2,
        pltpu.SemaphoreType.DMA((2, 2)),
        pltpu.SemaphoreType.DMA,
    )


def last_part(tick, a, y, wg, wu, wd, dgate, dup, grads):
    def body(g_tile, u_tile, d_tile, p, dgu, og, ou, od, in_sem, out_sem):
        dg, du = dgu.at[:, pl.ds(0, TILE)], dgu.at[:, pl.ds(TILE, TILE)]

        def ins(j):
            s = lax.rem(j, 2)
            pairs = ((wg.at[:, tile(j)], g_tile.at[s]), (wu.at[:, tile(j)], u_tile.at[s]), (wd.at[tile(j)], d_tile.at[s]))
            return [pltpu.make_async_copy(src, dst, in_sem.at[s, i]) for i, (src, dst) in enumerate(pairs)]

        def outs(j):
            pairs = ((og, grads["gate"].at[:, tile(j)]), (ou, grads["up"].at[:, tile(j)]), (od, grads["down"].at[tile(j)]))
            pairs += ((dg, dgate.at[:, tile(j)]), (du, dup.at[:, tile(j)]))
            return [pltpu.make_async_copy(src, dst, out_sem.at[i]) for i, (src, dst) in enumerate(pairs)]

        for c in ins(jnp.int32(0)):
            c.start()

        def go(j, carry):
            s = lax.rem(j, 2)
            for c in ins(j):
                c.wait()

            @pl.when(j < TILES - 1)
            def _():
                for c in ins(j + 1):
                    c.start()

            for half in range(2):
                rows = pl.ds(half * HALF, HALF)
                g, u = dot(a[rows, :], g_tile[s]), dot(a[rows, :], u_tile[s])
                dp = dot(y[rows, :], d_tile[s], NT).astype(BF16).astype(F32)
                p_, dg_, du_ = split(g, u, dp)
                p[rows, :], dgu[rows, :TILE], dgu[rows, TILE:] = p_.astype(BF16), dg_.astype(BF16), du_.astype(BF16)
            o = outs(j)
            o[3].start()
            o[4].start()
            tick(0, j, 0)
            both = dot(a[...], dgu[...], TN).astype(BF16)
            og[...], ou[...] = both[:, :TILE], both[:, TILE:]
            o[0].start()
            o[1].start()
            tick(0, j, 1)

            @pl.when(j > 0)
            def _():
                outs(j - 1)[2].wait()

            od[...] = dot(p[...], y[...], TN).astype(BF16)
            o[2].start()
            for i in (3, 4, 0, 1):
                o[i].wait()
            tick(0, j, 2)
            return carry

        lax.fori_loop(0, TILES, go, 0)
        outs(jnp.int32(TILES - 1))[2].wait()
        tick(0, None, 0)

    tiles = [pltpu.VMEM((2, D, TILE), BF16)] * 2 + [pltpu.VMEM((2, TILE, D), BF16)]
    pl.run_scoped(
        body,
        *tiles,
        pltpu.VMEM((T, TILE), BF16),
        pltpu.VMEM((T, 2 * TILE), BF16),
        *[pltpu.VMEM((D, TILE), BF16)] * 2,
        pltpu.VMEM((TILE, D), BF16),
        pltpu.SemaphoreType.DMA((2, 3)),
        pltpu.SemaphoreType.DMA((5,)),
    )


def states_part(tick, dgate, dup, wg, wu, h1, y, a, rows=256):
    n = T // rows

    def body(wg_all, wu_all, dg, du, sem, in_sem):
        first = [pltpu.make_async_copy(s, d, sem.at[i]) for i, (s, d) in enumerate(((wg, wg_all), (wu, wu_all)))]
        da = a.at[pl.ds(3 * rows, rows)]

        def at(j):
            return pl.ds(pl.multiple_of(j * rows, rows), rows)

        def ins(j):
            t = lax.rem(j, 3)
            pairs = ((dgate, dg), (dup, du), (h1, a.at[at(t)]))
            return [pltpu.make_async_copy(src.at[at(j)], dst, in_sem.at[i, t]) for i, (src, dst) in enumerate(pairs)]

        def back(j, slot):
            wide, grad = a[at(slot), :].astype(F32), da[...].astype(F32)
            scale = lax.rsqrt(jnp.mean(wide * wide, -1, keepdims=True) + 1e-6)
            inner = jnp.mean(grad * wide, -1, keepdims=True)
            dh = grad * scale - wide * (scale * scale * scale * inner)
            y[at(j), :] = (y[at(j), :].astype(F32) + dh).astype(BF16)

        def ahead(j, i):
            @pl.when(j < n - 1)
            def _():
                ins(j + 1)[i].start()

        start = ins(jnp.int32(0))
        for c in (start[0], first[0], start[1], first[1], start[2]):
            c.start()
        a[pl.ds(2 * rows, 2 * rows), :] = jnp.zeros((2 * rows, D), BF16)
        for c in first:
            c.wait()

        def go(j, carry):
            here = ins(j)
            here[2].wait()
            ahead(j, 2)
            here[0].wait()
            back(lax.max(j - 1, 0), lax.rem(j + 2, 3))
            by_gate = dot(dg[...], wg_all[...], NT)
            ahead(j, 0)
            here[1].wait()
            da[...] = (by_gate + dot(du[...], wu_all[...], NT)).astype(BF16)
            ahead(j, 1)
            tick(1, j, 0)
            return carry

        lax.fori_loop(0, n, go, 0)
        back(n - 1, (n - 1) % 3)
        tick(1, None, 0)

    pl.run_scoped(
        body,
        *[pltpu.VMEM((D, FF), BF16)] * 2,
        *[pltpu.VMEM((rows, FF), BF16)] * 2,
        pltpu.SemaphoreType.DMA((2,)),
        pltpu.SemaphoreType.DMA((3, 3)),
    )


def down0_part(tick, p0, y, grads):
    def body(p, od, in_sem, out_sem):
        def load(j):
            s = lax.rem(j, 2)
            return pltpu.make_async_copy(p0.at[:, tile(j)], p.at[s], in_sem.at[s])

        def out(j):
            return pltpu.make_async_copy(od, grads["down"].at[tile(j)], out_sem)

        load(jnp.int32(0)).start()

        def go(j, carry):
            s = lax.rem(j, 2)
            load(j).wait()

            @pl.when(j < TILES - 1)
            def _():
                load(j + 1).start()

            @pl.when(j > 0)
            def _():
                out(j - 1).wait()

            od[...] = dot(p[s], y[...], TN).astype(BF16)
            out(j).start()
            tick(2, j, 0)
            return carry

        lax.fori_loop(0, TILES, go, 0)
        out(jnp.int32(TILES - 1)).wait()
        tick(2, None, 0)

    pl.run_scoped(
        body,
        pltpu.VMEM((2, T, TILE), BF16),
        pltpu.VMEM((TILE, D), BF16),
        pltpu.SemaphoreType.DMA((2,)),
        pltpu.SemaphoreType.DMA,
    )


def first_part(tick, a, y, wd, gate0, up0, grads):
    def body(d_tile, g, u, dgu, og, ou, in_sem, out_sem):
        def ins(j):
            s = lax.rem(j, 2)
            pairs = ((wd.at[tile(j)], d_tile.at[s]), (gate0.at[:, tile(j)], g.at[s]), (up0.at[:, tile(j)], u.at[s]))
            return [pltpu.make_async_copy(src, dst, in_sem.at[s, i]) for i, (src, dst) in enumerate(pairs)]

        def outs(j):
            pairs = ((og, grads["gate"].at[:, tile(j)]), (ou, grads["up"].at[:, tile(j)]))
            return [pltpu.make_async_copy(src, dst, out_sem.at[i]) for i, (src, dst) in enumerate(pairs)]

        for c in ins(jnp.int32(0)):
            c.start()

        def go(j, carry):
            s = lax.rem(j, 2)
            for c in ins(j):
                c.wait()

            @pl.when(j < TILES - 1)
            def _():
                for c in ins(j + 1):
                    c.start()

            for half in range(2):
                rows = pl.ds(half * HALF, HALF)
                dp = dot(y[rows, :], d_tile[s], NT).astype(BF16).astype(F32)
                _, dg_, du_ = split(g[s, rows, :], u[s, rows, :], dp)
                dgu[rows, :TILE], dgu[rows, TILE:] = dg_.astype(BF16), du_.astype(BF16)

            @pl.when(j > 0)
            def _():
                for c in outs(j - 1):
                    c.wait()

            tick(3, j, 0)
            both = dot(a[...], dgu[...], TN).astype(BF16)
            og[...], ou[...] = both[:, :TILE], both[:, TILE:]
            for c in outs(j):
                c.start()
            tick(3, j, 1)
            return carry

        lax.fori_loop(0, TILES, go, 0)
        for c in outs(jnp.int32(TILES - 1)):
            c.wait()
        tick(3, None, 0)

    pl.run_scoped(
        body,
        pltpu.VMEM((2, TILE, D), BF16),
        *[pltpu.VMEM((2, T, TILE), F32)] * 2,
        pltpu.VMEM((T, 2 * TILE), BF16),
        *[pltpu.VMEM((D, TILE), BF16)] * 2,
        pltpu.SemaphoreType.DMA((2, 3)),
        pltpu.SemaphoreType.DMA((2,)),
    )


def finish(whole, sums, m, v):
    slots, jobs = 6, 8

    def kernel(*refs):
        srcs, refs = refs[:3], refs[3:]
        ins, outs = refs[:9], refs[9:18]
        buffers, (in_sem, out_sem) = refs[18:20], refs[20:]
        queue = [(i, n) for n in range(jobs) for i in range(3)]
        used, loads, stores = [0, 0], [], []
        for i, n in queue:
            buffer = buffers[i // 2]
            slot = used[i // 2] % buffer.shape[0]
            used[i // 2] += 1
            rows = pl.ds(n * buffer.shape[1], buffer.shape[1])
            sems = (in_sem.at[i // 2, slot], out_sem.at[i // 2, slot])
            loads.append(pltpu.make_async_copy(srcs[i].at[rows], buffer.at[slot], sems[0]))
            stores.append(pltpu.make_async_copy(buffer.at[slot], outs[i].at[rows], sems[1]))
        ahead = 2 * slots - slots // 2
        for c in loads[:ahead]:
            c.start()
        for g, m_ref, v_ref, new_m, new_v in zip(*(ins[3 * i :][:3] for i in range(3)), outs[3:6], outs[6:9]):
            for layer in range(2):
                at = (slice(None), layer) if m_ref.shape[1] == 2 else (layer,)
                grad = g[layer].astype(F32)
                new_m[at] = 0.9 * m_ref[at] + 0.1 * grad
                new_v[at] = 0.95 * v_ref[at] + 0.05 * grad * grad
        for n, (load, store) in enumerate(zip(loads, stores)):
            load.wait()
            store.start()
            if n >= 3 and n + ahead - 3 < len(loads):
                stores[n - 3].wait()
                loads[n + ahead - 3].start()
        for n, store in enumerate(stores):
            if n + ahead >= len(loads):
                store.wait()

    tall = [t.reshape(-1, t.shape[-1]) for t in whole]
    shapes = [jax.ShapeDtypeStruct(t.shape, t.dtype) for t in (*tall, *m, *v)]
    hbm = pl.BlockSpec(memory_space=pl.ANY)
    vmem = pl.BlockSpec(memory_space=pltpu.VMEM)
    buffers = [pltpu.VMEM((slots, 2 * D // jobs, FF), BF16), pltpu.VMEM((slots // 2, 2 * FF // jobs, D), BF16)]
    out = pl.pallas_call(
        kernel,
        out_shape=shapes,
        in_specs=[hbm] * 3 + [vmem] * 9,
        out_specs=[hbm] * 3 + [vmem] * 6,
        scratch_shapes=buffers + [pltpu.SemaphoreType.DMA((2, slots))] * 2,
        compiler_params=pltpu.CompilerParams(vmem_limit_bytes=67043328),
        name="finish",
    )(*tall, *sums, *m, *v)
    return [t.reshape(2, -1, t.shape[-1]) for t in out[:3]], out[3:6], out[6:]


def turned(t):
    return (*t[:2], jnp.swapaxes(t[2], 0, 1))


def step(x, dy, *arrays):
    weights, m, v = (arrays[i : i + 3] for i in (0, 3, 6))
    x, dy, m, v = x[0], dy[0], turned(m), turned(v)
    block = lax.dynamic_slice_in_dim(weights[2], lax.axis_index("dp") * 22, 22, 1)
    whole, sums = train(x, dy, weights, block, m, v)
    new_w, new_m, new_v = finish(whole, sums, m, v)
    return (*new_w, *turned(new_m), *turned(new_v))


def solution(mesh):
    P = jax.sharding.PartitionSpec
    data, state = P(("rep", "dp")), P(None, "dp")
    return jax.shard_map(
        step,
        mesh=mesh,
        in_specs=(data, data, P(), P(), P(), *[state] * 6),
        out_specs=(*[P("rep")] * 3, *[P("rep", "dp")] * 6),
        check_vma=False,
    )
```

```python
import functools

import jax
import jax.numpy as jnp
from jax import lax
from jax.experimental import pallas as pl
from jax.experimental.pallas import tpu as pltpu

LOGICAL = pl.DeviceIdType.LOGICAL
F32, BF16 = jnp.float32, jnp.bfloat16
T, D, FF = 2048, 1024, 2816
SIZE = {"x": 4, "y": 4, "z": 8}
STRIDE = {"x": 32, "y": 8, "z": 1}
PARTNERS = 13
MESSAGES = 39


class Place:
    def __init__(self):
        me = self.me = lax.axis_index("dp")
        self.at = {"x": me // 32, "y": (me // 8) % 4, "z": me % 8}
        self.number = lax.axis_index("rep") * 128 + me
        self.ring = {(axis, step): (self.at_step(axis, step), self.partner(axis, step)) for axis in "xyz" for step in (1, -1)}

    def at_step(self, axis, step):
        return lax.rem(self.at[axis] + (step + SIZE[axis] if isinstance(step, int) else step), SIZE[axis])

    def chunk(self, axis, step):
        return self.at[axis] if isinstance(step, int) and step == 0 else self.at_step(axis, step)

    def partner(self, axis, step):
        return self.number + (self.at_step(axis, step) - self.at[axis]) * STRIDE[axis]

    def tell(self, semaphore):
        for axis, n in SIZE.items():

            def one(step, c, axis=axis):
                pl.semaphore_signal(semaphore, inc=1, device_id=self.partner(axis, step), device_id_type=LOGICAL)
                return c

            lax.fori_loop(1, n, one, 0)

    def greet(self):
        barrier = pltpu.get_barrier_semaphore()
        self.tell(barrier)
        pl.semaphore_wait(barrier, PARTNERS)


class Action:
    def __init__(self, waits, do, sends, cost=0.3, frees=False):
        self.waits, self.do, self.sends, self.cost, self.frees = waits, do, sends, cost, frees


class Chain:
    def __init__(self, actions, release, before=None):
        self.actions, self.release, self.before, self.done, self.freed = actions, release, before, 0, None

    def ended(self):
        return self.done == len(self.actions)


RATE = 45.5e3


LATENCY = 3.5


def plan(chains, ticks, latency=LATENCY):
    free, arrive, now, placed, rest = {}, {}, 0.0, [], []

    def run(c, a, at):
        if a.frees:
            c.freed = at
        for name, link, nbytes, further in a.sends:
            begin = max(free.get(link, 0.0), at + a.cost)
            free[link] = begin + nbytes / RATE
            arrive[name] = free[link] + latency + further

    def ready(c, tick):
        if c.ended() or c.release > tick or (c.before and c.before.freed is None):
            return None
        waits = c.actions[c.done].waits
        known = [arrive[w] for w in waits if w in arrive] + [c.before.freed + latency if c.before else 0.0]
        return max(known) if len(known) > len(waits) else None

    for tick, time in enumerate(ticks):
        now += time
        here = []
        while True:
            best = min(((r, i) for i, c in enumerate(chains) if (r := ready(c, tick)) is not None and r <= now), default=None)
            if best is None:
                break
            c = chains[best[1]]
            a = c.actions[c.done]
            c.done += 1
            run(c, a, now)
            now += a.cost
            here.append(a)
        placed.append(here)
    while not all(c.ended() for c in chains):
        r, i = min((max(r, now), i) for i, c in enumerate(chains) if (r := ready(c, len(ticks))) is not None)
        c = chains[i]
        a = c.actions[c.done]
        c.done += 1
        now = max(r, now)
        run(c, a, now)
        now += a.cost
        rest.append(a)
    return placed, rest, now


def volume(shape):
    n = 2
    for v in shape:
        n *= v
    return n


def each(shape, f):
    if len(shape) > 3 or shape[-2] == 176 and len(shape) == 3:
        lax.fori_loop(0, shape[0], lambda i, c: (f((i,)), c)[1], 0)
    else:
        f((slice(None),) * len(shape))


class Strip:
    def __init__(self, kind, start, width, role, axes):
        self.kind, self.start, self.width, self.role, self.axes = kind, start, width, role, axes
        self.cols = pl.ds(start, width)
        left = [a for a in "xyz" if a != axes[0]]
        if kind == "down":
            shapes = ((4, 176), (176,), (24,))
        else:
            shapes = ((SIZE[left[0]], SIZE[left[1]], 8), (SIZE[left[1]], 8), (8,))
        self.shapes = [(*s, width) for s in shapes]
        self.back = axes[::-1]
        n = SIZE[axes[0]]
        self.far = {1: n // 2 if role == 0 else n // 2 - 1, -1: n // 2 if role == 1 else n // 2 - 1}
        self.ring = [(d, k) for d in (1, -1) for k in range(self.far[d], 0, -1)]
        self.counts = [SIZE[a] - 1 for a in (*axes, *self.back)]
        sums = {d: [d * k for k in range(self.far[d] - 1, 0, -1)] for d in (1, -1)}
        short = -1 if role == 0 else 1
        sums[short] = sums[short] + [0]
        self.own = [sums[-short] + sums[short]] if n == 4 else [sums[1], sums[-1]]

    def offset(self, layer, what, i):
        if what == "rs":
            return sum(self.counts[:i])
        return sum(self.counts[: 3 + i]) + layer * sum(self.counts[3:])

    def scratch(self):
        s = {"own": pltpu.VMEM((len(self.own), *self.shapes[0]), BF16), "acc1": pltpu.VMEM(self.shapes[1], F32)}
        s["acc2"] = pltpu.VMEM((SIZE[self.axes[2]], *self.shapes[2]), F32)
        for i in range(3):
            s[f"recv{i}"] = pltpu.VMEM((self.counts[i], *self.shapes[i]), BF16)
        for i in (1, 2):
            s[f"send{i}"] = pltpu.VMEM((self.counts[i], *self.shapes[i]), BF16)
        if self.kind == "down":
            s["flat"] = pltpu.VMEM(self.shapes[1], F32)
            s["blocks"] = pltpu.VMEM((2, 8, *self.shapes[2]), BF16)
            s["rows"] = pltpu.VMEM((2, *self.shapes[1]), BF16)
        return s

    def chain(self, place, layer, grad, new, out, refs, sems, update):
        send_sem, recv_sem, local_sem, free_sem, place_of = sems
        axes, back, shapes, cols = self.axes, self.back, self.shapes, self.cols
        base, first_local = place_of * MESSAGES, place_of * 6

        def name(*m):
            return (layer, id(self), *m)

        def raw(step):
            c = place.chunk(axes[0], step)
            if self.kind == "down":
                return grad.at[c, :, :, cols] if axes[0] == "x" else grad.at[:, c, :, cols]
            return grad.at[(*(c if a == axes[0] else slice(None) for a in "xyz"), slice(None), cols)]

        def received(d, k):
            return refs["recv0"].at[self.ring.index((d, k))]

        def source(d, k):
            return received(d, k + 1) if k < self.far[d] else raw(d * k)

        def part(i, step):
            c = place.chunk(back[i], step)
            if self.kind == "down" and i == 0:
                return refs["blocks"].at[layer, c]
            known = {a: (slice(None) if a in back[:i] else c if a == back[i] else place.chunk(a, 0)) for a in "xyz"}
            if self.kind == "down":
                return out.at[known["x"], known["y"], :, cols]
            return out.at[known["x"], known["y"], known["z"], :, cols]

        def like(what, i):
            return refs[f"recv{i}"].at[0] if what == "rs" else part(i, 0)

        def send(what, i, n, src, dst, device):
            n = base + self.offset(layer, what, i) + n
            pltpu.make_async_remote_copy(src, dst, send_sem.at[n], recv_sem.at[n], device_id=device, device_id_type=LOGICAL).start()

        def wait(sem, what, i, n):
            ref = like(what, i)
            pltpu.make_async_copy(ref, ref, sem.at[base + self.offset(layer, what, i) + n]).wait()

        def wait_all(sem, what, i):
            count = self.counts[i if what == "rs" else 3 + i]
            lax.fori_loop(0, count, lambda n, c: (wait(sem, what, i, n), c)[1], 0)

        def ring_send(d, k):
            send("rs", 0, self.ring.index((d, k)), source(d, k), received(d, k), place.ring[axes[0], d][1])

        def ring_back(d, k):
            there = part(2, -d * (k - 1))
            send("ag", 2, self.ring.index((d, k)), there, there, place.ring[back[2], d][1])

        def to_each(what, i, f):
            axis = (axes if what == "rs" else back)[i]

            def one(step, c):
                send(what, i, step - 1, *f(step), place.partner(axis, step))
                return c

            lax.fori_loop(1, SIZE[axis], one, 0)

        def own_copy(step):
            b = next(b for b, seq in enumerate(self.own) if step in seq)
            return pltpu.make_async_copy(raw(step), refs["own"].at[b], local_sem.at[first_local + b])

        def own(step):
            b = next(b for b, seq in enumerate(self.own) if step in seq)
            mine = refs["own"].at[b]
            pltpu.make_async_copy(mine, mine, local_sem.at[first_local + b]).wait()
            return mine

        def begin():
            if layer == 0:
                for i in (1, 2):
                    wait_all(send_sem, "rs", i)
                for d in (1, -1):
                    wait(send_sem, "rs", 0, self.ring.index((d, self.far[d])))
                pl.semaphore_wait(free_sem.at[place_of], PARTNERS)
            for d in (1, -1):
                ring_send(d, self.far[d])
            for seq in self.own:
                own_copy(seq[0]).start()

        def add(d, k):
            wait(recv_sem, "rs", 0, self.ring.index((d, k + 1)))
            theirs, mine = received(d, k + 1), own(d * k)

            def f(at):
                theirs[at] = (mine[at].astype(F32) + theirs[at].astype(F32)).astype(BF16)

            each(shapes[0], f)
            for seq in self.own:
                if d * k in seq[:-1]:
                    own_copy(seq[seq.index(d * k) + 1]).start()
            ring_send(d, k)

        def end_0():
            mine = own(0)
            for d in (1, -1):
                wait(recv_sem, "rs", 0, self.ring.index((d, 1)))

            def total(step):
                c = place.chunk(axes[1], step)
                return mine[c].astype(F32) + received(1, 1)[c].astype(F32) + received(-1, 1)[c].astype(F32)

            def f(step):
                to = refs["send1"].at[step - 1]
                to[...] = total(step).astype(BF16)
                return to, refs["recv1"].at[step - 1]

            to_each("rs", 1, f)
            refs["acc1"][...] = total(0)

        def end_1():
            wait_all(recv_sem, "rs", 1)
            acc2 = refs["acc2"]
            total = refs["acc1"][...]
            for n in range(self.counts[1]):
                total = total + refs["recv1"][n].astype(F32)
            if self.kind == "down":
                refs["flat"][...] = total
                for z in range(8):
                    acc2[z, :22, :] = refs["flat"][22 * z : 22 * z + 22, :]
            else:
                acc2[...] = total

            def f(step):
                to = refs["send2"].at[step - 1]
                to[...] = acc2[place.chunk(axes[2], step)].astype(BF16)
                return to, refs["recv2"].at[step - 1]

            to_each("rs", 2, f)

        def end_2():
            wait_all(recv_sem, "rs", 2)
            mine = refs["acc2"][place.chunk(axes[2], 0)]
            update(lax.fori_loop(0, self.counts[2], lambda n, t: t + refs["recv2"][n].astype(F32), mine))
            if layer == 1:
                for d, k in self.ring:
                    if k < self.far[d]:
                        wait(send_sem, "rs", 0, self.ring.index((d, k)))
                place.tell(free_sem.at[place_of])
            mine_copy(0).start()
            to_each("ag", 0, lambda step: (new.at[:, cols], part(0, 0)))

        def mine_copy(i):
            return pltpu.make_async_copy(new.at[:, cols] if i == 0 else refs["rows"].at[layer], part(i, 0), local_sem.at[first_local + 2 + 2 * layer + i])

        def next_back(i):
            wait_all(recv_sem, "ag", i - 1)
            if i == 1:
                mine_copy(0).wait()
            if self.kind == "down":
                if i == 1:
                    for z in range(8):
                        refs["flat"][22 * z : 22 * z + 22, :] = refs["blocks"][layer, z, :22, :].astype(F32)
                    refs["rows"][layer] = refs["flat"][...].astype(BF16)
                    mine_copy(1).start()
                else:
                    mine_copy(1).wait()
            if i == 1:
                to_each("ag", 1, lambda step: (refs["rows"].at[layer] if self.kind == "down" else part(1, 0), part(1, 0)))
            else:
                for d in (1, -1):
                    ring_back(d, 1)

        def forward(d, k):
            wait(recv_sem, "ag", 2, self.ring.index((d, k - 1)))
            ring_back(d, k)

        def finish():
            for d in (1, -1):
                wait(recv_sem, "ag", 2, self.ring.index((d, self.far[d])))
            for i in range(3):
                wait_all(send_sem, "ag", i)
                if layer == 0:
                    wait_all(send_sem, "rs", i)

        def listed(what, i, ms):
            axis = (axes if what == "rs" else back)[i]
            held = 8
            for a in back[:i]:
                held *= SIZE[a]
            nbytes = volume(shapes[i]) if what == "rs" else 2 * self.width * ((24, 176, 704)[i] if self.kind == "down" else held)
            n, found = SIZE[axis], []
            for d, k in ms:
                hops = 1 if d else min(k, n - k)
                way = d or (1 if 2 * k < n or 2 * k == n and self.role == 0 else -1)
                found.append((name(what, i, d, k), (axis, way), nbytes * hops, 0.7 * (hops - 1)))
            return found

        def all_of(what, i):
            return [(0, k) for k in range(1, self.counts[i if what == "rs" else 3 + i] + 1)]

        def names(what, i, ms):
            return [name(what, i, *m) for m in ms]

        far = self.far
        todo = [Action([], begin, listed("rs", 0, [(d, far[d]) for d in (1, -1)]), 0.03)]
        for k in range(max(far.values()) - 1, 0, -1):
            for d in (1, -1):
                if k < far[d]:
                    todo.append(Action([name("rs", 0, d, k + 1)], functools.partial(add, d, k), listed("rs", 0, [(d, k)]), 0.15 if SIZE[axes[0]] == 4 else 0.07))
        todo.append(Action(names("rs", 0, [(1, 1), (-1, 1)]), end_0, listed("rs", 1, all_of("rs", 1)), 0.2))
        todo.append(Action(names("rs", 1, all_of("rs", 1)), end_1, listed("rs", 2, all_of("rs", 2)), 0.2))
        todo.append(Action(names("rs", 2, all_of("rs", 2)), end_2, listed("ag", 0, all_of("ag", 0)), 0.45, True))
        todo.append(Action(names("ag", 0, all_of("ag", 0)), functools.partial(next_back, 1), listed("ag", 1, all_of("ag", 1)), 0.12))
        todo.append(Action(names("ag", 1, all_of("ag", 1)), functools.partial(next_back, 2), listed("ag", 2, [(1, 1), (-1, 1)]), 0.06))
        for k in range(2, max(far.values()) + 1):
            for d in (1, -1):
                if k <= far[d]:
                    todo.append(Action([name("ag", 2, d, k - 1)], functools.partial(forward, d, k), listed("ag", 2, [(d, k)]), 0.03))
        todo.append(Action(names("ag", 2, [(d, far[d]) for d in (1, -1)]), finish, [], 0.15))
        return todo


NN = (((1,), (0,)), ((), ()))
NT = (((1,), (1,)), ((), ()))
TN = (((0,), (0,)), ((), ()))
KINDS = ("gate", "up", "down")
ROWS = {"gate": 8, "up": 8, "down": 22}
VIEWS = {"gate": (4, 4, 8, 8, FF), "up": (4, 4, 8, 8, FF), "down": (4, 4, 176, D)}
TILE = 256
TILES = FF // TILE
HALF = T // 2


def dot(a, b, dims=NN):
    return lax.dot_general(a, b, dims, preferred_element_type=F32)


def normed(h):
    wide = h.astype(F32)
    return (wide * lax.rsqrt(jnp.mean(wide * wide, -1, keepdims=True) + 1e-6)).astype(BF16)


def split(g, u, dp):
    s = jax.nn.sigmoid(g)
    silu = g * s
    return silu * u, dp * u * (s + silu * (1 - s)), dp * silu


def tile(j):
    return pl.ds(pl.multiple_of(j * TILE, TILE), TILE)


LAST = (TILES, (4.2, 2.1, 1.45))
STATES = (8, (4.6,))
DOWN0 = (TILES, (1.9,))
FIRST = (TILES, (2.25, 2.45))
PARTS = (LAST, STATES, DOWN0, FIRST)


def tick_list():
    times, starts = [], []
    for n, each_time in PARTS:
        starts.append(len(times))
        times += list(each_time) * n
        times.append(0.5)
    return times, starts


STRIPS = [
    ("gate", 0, 512, 1, "zxy"),
    ("up", 0, 512, 1, "xyz"),
    ("gate", 512, 512, 1, "zxy"),
    ("up", 512, 512, 1, "yxz"),
    ("gate", 1024, 768, 0, "xyz"),
    ("up", 1024, 768, 0, "yxz"),
    ("gate", 1792, 512, 0, "zxy"),
    ("up", 1792, 512, 1, "yxz"),
    ("gate", 2304, 512, 1, "zxy"),
    ("up", 2304, 512, 0, "zxy"),
    ("down", 0, 256, 1, "yxz"),
    ("down", 256, 256, 0, "yxz"),
    ("down", 512, 256, 0, "xyz"),
    ("down", 768, 256, 1, "xyz"),
]


def releases(layer, strip, starts):
    last_tile = (strip.start + strip.width) // TILE - 1
    if layer == 1:
        n = len(LAST[1])
        return starts[0] + (TILES * n if strip.kind == "down" or last_tile == TILES - 1 else last_tile * n + n - 1)
    if strip.kind == "down":
        return starts[2] + TILES * len(DOWN0[1])
    n = len(FIRST[1])
    return starts[3] + (TILES * n if last_tile == TILES - 1 else (last_tile + 1) * n)


def make_strips():
    return [Strip(*s) for s in STRIPS]


def train(x, dy, weights, block, m, v):
    strips = make_strips()
    n_messages = MESSAGES * len(strips)
    scratch, names = [], []
    for s in strips:
        for k, shape in s.scratch().items():
            names.append((s, k))
            scratch.append(shape)

    def kernel(*refs):
        x, dy, wg, wu, wd = refs[:5]
        m, v = (dict(zip(KINDS, refs[6 + 3 * i :])) for i in range(2))
        outs, sums = (dict(zip(KINDS, refs[12 + 3 * i :])) for i in range(2))
        grads = [dict(zip(KINDS, refs[18 + 3 * i :])) for i in range(2)]
        dgate, dup, p0, gate0, up0, a0, h1 = refs[24:31]
        old = {"gate": refs[31], "up": refs[32], "down": refs[5]}
        refs = refs[33:]
        new = dict(zip(KINDS, refs))
        send_sem, recv_sem, local_sem, free_sem, old_sem = refs[3:8]
        refs = refs[8:]
        place = Place()
        mine = pl.ds(pl.multiple_of(place.me * 8, 8), 8)
        loads = [pltpu.make_async_copy(w.at[:, mine], old[k], old_sem.at[i]) for i, (k, w) in enumerate((("gate", wg), ("up", wu)))]
        for c in loads:
            c.start()
        barrier = pltpu.get_barrier_semaphore()
        place.tell(barrier)
        for c in loads:
            c.wait()
        new["down"][...] = jnp.zeros(new["down"].shape, BF16)
        times, starts = tick_list()
        chains, before = [], {}
        for n, s in enumerate(strips):
            mine = {k: r for (t, k), r in zip(names, refs) if t is s}
            for layer in (1, 0):

                def update(g, s=s, layer=layer):
                    rows = ROWS[s.kind]
                    at = (layer, pl.ds(0, rows), s.cols)
                    g = g[:rows].astype(BF16)
                    sums[s.kind][at] = g
                    g = g.astype(F32)
                    w = old[s.kind][at].astype(F32)
                    moments_at = (at[1], layer, s.cols) if s.kind == "down" else at
                    m1 = 0.9 * m[s.kind][moments_at] + 0.1 * g
                    v1 = 0.95 * v[s.kind][moments_at] + 0.05 * g * g
                    new[s.kind][at] = (w - 0.02 * (m1 * lax.rsqrt(v1 + 1e-8) + 0.1 * w)).astype(BF16)

                grad = grads[layer][s.kind].reshape(*VIEWS[s.kind])
                sems = (send_sem, recv_sem, local_sem, free_sem, n)
                a = s.chain(place, layer, grad, new[s.kind].at[layer], outs[s.kind].at[layer], mine, sems, update)
                chains.append(Chain(a, releases(layer, s, starts), before.get(s)))
                before[s] = chains[-1]
        placed, rest, _ = plan(chains, times)

        def tick(part, j, i):
            n, each_time = PARTS[part]
            per = len(each_time)
            if j is None:
                for a in placed[starts[part] + n * per]:
                    a.do()
                return
            for when in range(n):
                here = placed[starts[part] + when * per + i]
                if here:

                    @pl.when(j == when)
                    def _(here=here):
                        for a in here:
                            a.do()

        def parts(a, y, sem):
            load = pltpu.make_async_copy(dy, y, sem)
            load.start()
            forward_part(x, wg.at[0], wu.at[0], wd.at[0], a0, gate0, up0, p0, h1, a)
            load.wait()
            pl.semaphore_wait(barrier, PARTNERS)

            def last_layer(w, w_sem):
                load = pltpu.make_async_copy(wg.at[1], w, w_sem)
                load.start()
                last_part(tick, a, y, wg.at[1], wu.at[1], wd.at[1], dgate, dup, grads[1])
                load.wait()
                states_part(tick, dgate, dup, w, wu.at[1], h1, y, a)

            pl.run_scoped(last_layer, pltpu.VMEM((D, FF), BF16), pltpu.SemaphoreType.DMA)
            load = pltpu.make_async_copy(a0, a, sem)
            load.start()
            down0_part(tick, p0, y, grads[0])
            load.wait()
            first_part(tick, a, y, wd.at[0], gate0, up0, grads[0])

        pl.run_scoped(parts, *[pltpu.VMEM((T, D), BF16)] * 2, pltpu.SemaphoreType.DMA)
        for a in rest:
            a.do()

    hbm = pl.BlockSpec(memory_space=pl.ANY)
    vmem = pl.BlockSpec(memory_space=pltpu.VMEM)
    wide = [jax.ShapeDtypeStruct((2, *VIEWS[k]), BF16) for k in KINDS]
    own = [jax.ShapeDtypeStruct((2, ROWS[k], VIEWS[k][-1]), BF16) for k in KINDS]
    local = [jax.ShapeDtypeStruct((FF, D) if k == "down" else (D, FF), BF16) for _ in range(2) for k in KINDS]
    local += [jax.ShapeDtypeStruct((T, FF), t) for t in (BF16, BF16, BF16, F32, F32)] + [jax.ShapeDtypeStruct((T, D), BF16)] * 2
    out = pl.pallas_call(
        kernel,
        out_shape=wide + own + local,
        in_specs=[hbm] * 5 + [vmem] * 7,
        out_specs=[hbm] * 3 + [vmem] * 3 + [hbm] * 13,
        scratch_shapes=[pltpu.VMEM((2, 8, FF), BF16)] * 2
        + [pltpu.VMEM((2, -(-ROWS[k] // 8) * 8, VIEWS[k][-1]), BF16) for k in KINDS]
        + [pltpu.SemaphoreType.DMA((n_messages,))] * 2
        + [pltpu.SemaphoreType.DMA((6 * len(strips),)), pltpu.SemaphoreType.REGULAR((len(strips),)), pltpu.SemaphoreType.DMA((2,))]
        + scratch,
        compiler_params=pltpu.CompilerParams(collective_id=1, has_side_effects=True, vmem_limit_bytes=67043328),
        name="train",
    )(x, dy, *weights, block, *m, *v)
    return out[:3], out[3:6]


def forward_part(x, wg, wu, wd, a0, gate0, up0, p0, h1, a):
    rows, tall = 256, 512
    n, n_tall = T // rows, T // tall

    def at(j, rows=rows):
        return pl.ds(pl.multiple_of(j * rows, rows), rows)

    def body(g_tile, u_tile, in_sem, a_sem):
        store_a = pltpu.make_async_copy(a, a0, a_sem)

        def ins(j):
            s = lax.rem(j, 2)
            pairs = ((wg, g_tile), (wu, u_tile))
            return [pltpu.make_async_copy(src.at[:, tile(j)], dst.at[s], in_sem.at[s, i]) for i, (src, dst) in enumerate(pairs)]

        def norm(h, sem):
            def load(j):
                return pltpu.make_async_copy(x.at[at(j)], h.at[at(j)], sem.at[j])

            lax.fori_loop(0, n, lambda j, c: (load(j).start(), c)[1], 0)
            for c in ins(jnp.int32(0)):
                c.start()

            def go(j, carry):
                load(j).wait()
                a[at(j), :] = normed(h[at(j), :])
                return carry

            lax.fori_loop(0, n, go, 0)

        def gates(g, u, p, out_sem):
            def outs(j):
                s = lax.rem(j, 2)
                pairs = ((g, gate0), (u, up0), (p, p0))
                return [pltpu.make_async_copy(src.at[s], dst.at[:, tile(j)], out_sem.at[s, i]) for i, (src, dst) in enumerate(pairs)]

            def go(j, carry):
                s = lax.rem(j, 2)
                for c in ins(j):
                    c.wait()

                @pl.when(j < TILES - 1)
                def _():
                    for c in ins(j + 1):
                        c.start()

                @pl.when(j > 1)
                def _():
                    for c in outs(j - 2):
                        c.wait()

                for half in range(2):
                    rows = pl.ds(half * HALF, HALF)
                    gate, up = dot(a[rows, :], g_tile[s]), dot(a[rows, :], u_tile[s])
                    g[s, rows, :], u[s, rows, :] = gate, up
                    p[s, rows, :] = (gate * jax.nn.sigmoid(gate) * up).astype(BF16)
                for c in outs(j):
                    c.start()
                return carry

            lax.fori_loop(0, TILES, go, 0)
            for j in (TILES - 2, TILES - 1):
                for c in outs(jnp.int32(j)):
                    c.wait()

        def next_states(w, p, h, o, w_sem, sem, out_sem):
            load_w = pltpu.make_async_copy(wd, w, w_sem)
            def loads(j):
                s = lax.rem(j, 2)
                return [pltpu.make_async_copy(src.at[at(j, tall)], dst.at[s], sem.at[s, i]) for i, (src, dst) in enumerate(((p0, p), (x, h)))]

            def out(j):
                s = lax.rem(j, 2)
                return pltpu.make_async_copy(o.at[s], h1.at[at(j, tall)], out_sem.at[s])

            for c in (load_w, *loads(jnp.int32(0))):
                c.start()
            store_a.wait()
            load_w.wait()

            def go(j, carry):
                s = lax.rem(j, 2)
                for c in loads(j):
                    c.wait()

                @pl.when(j < n_tall - 1)
                def _():
                    for c in loads(j + 1):
                        c.start()

                @pl.when(j > 1)
                def _():
                    out(j - 2).wait()

                a[at(lax.max(j - 1, 0), tall), :] = normed(o[1 - s])
                o[s] = h[s] + dot(p[s], w[...]).astype(BF16)
                out(j).start()
                return carry

            o[1] = jnp.zeros((tall, D), BF16)
            lax.fori_loop(0, n_tall, go, 0)
            a[at(n_tall - 1, tall), :] = normed(o[(n_tall - 1) % 2])
            for j in (n_tall - 2, n_tall - 1):
                out(jnp.int32(j)).wait()

        pl.run_scoped(norm, pltpu.VMEM((T, D), BF16), pltpu.SemaphoreType.DMA((n,)))
        store_a.start()
        stores = [pltpu.VMEM((2, T, TILE), t) for t in (F32, F32, BF16)]
        pl.run_scoped(gates, *stores, pltpu.SemaphoreType.DMA((2, 3)))
        tiles = [pltpu.VMEM((FF, D), BF16), pltpu.VMEM((2, tall, FF), BF16), pltpu.VMEM((2, tall, D), BF16), pltpu.VMEM((2, tall, D), BF16)]
        pl.run_scoped(next_states, *tiles, pltpu.SemaphoreType.DMA, pltpu.SemaphoreType.DMA((2, 2)), pltpu.SemaphoreType.DMA((2,)))

    pl.run_scoped(
        body,
        *[pltpu.VMEM((2, D, TILE), BF16)] * 2,
        pltpu.SemaphoreType.DMA((2, 2)),
        pltpu.SemaphoreType.DMA,
    )


def last_part(tick, a, y, wg, wu, wd, dgate, dup, grads):
    def body(g_tile, u_tile, d_tile, p, dgu, og, ou, od, in_sem, out_sem):
        dg, du = dgu.at[:, pl.ds(0, TILE)], dgu.at[:, pl.ds(TILE, TILE)]

        def ins(j):
            s = lax.rem(j, 2)
            pairs = ((wg.at[:, tile(j)], g_tile.at[s]), (wu.at[:, tile(j)], u_tile.at[s]), (wd.at[tile(j)], d_tile.at[s]))
            return [pltpu.make_async_copy(src, dst, in_sem.at[s, i]) for i, (src, dst) in enumerate(pairs)]

        def outs(j):
            pairs = ((og, grads["gate"].at[:, tile(j)]), (ou, grads["up"].at[:, tile(j)]), (od, grads["down"].at[tile(j)]))
            pairs += ((dg, dgate.at[:, tile(j)]), (du, dup.at[:, tile(j)]))
            return [pltpu.make_async_copy(src, dst, out_sem.at[i]) for i, (src, dst) in enumerate(pairs)]

        for c in ins(jnp.int32(0)):
            c.start()

        def go(j, carry):
            s = lax.rem(j, 2)
            for c in ins(j):
                c.wait()

            @pl.when(j < TILES - 1)
            def _():
                for c in ins(j + 1):
                    c.start()

            for half in range(2):
                rows = pl.ds(half * HALF, HALF)
                g, u = dot(a[rows, :], g_tile[s]), dot(a[rows, :], u_tile[s])
                dp = dot(y[rows, :], d_tile[s], NT).astype(BF16).astype(F32)
                p_, dg_, du_ = split(g, u, dp)
                p[rows, :], dgu[rows, :TILE], dgu[rows, TILE:] = p_.astype(BF16), dg_.astype(BF16), du_.astype(BF16)
            o = outs(j)
            o[3].start()
            o[4].start()
            tick(0, j, 0)
            both = dot(a[...], dgu[...], TN).astype(BF16)
            og[...], ou[...] = both[:, :TILE], both[:, TILE:]
            o[0].start()
            o[1].start()
            tick(0, j, 1)

            @pl.when(j > 0)
            def _():
                outs(j - 1)[2].wait()

            od[...] = dot(p[...], y[...], TN).astype(BF16)
            o[2].start()
            for i in (3, 4, 0, 1):
                o[i].wait()
            tick(0, j, 2)
            return carry

        lax.fori_loop(0, TILES, go, 0)
        outs(jnp.int32(TILES - 1))[2].wait()
        tick(0, None, 0)

    tiles = [pltpu.VMEM((2, D, TILE), BF16)] * 2 + [pltpu.VMEM((2, TILE, D), BF16)]
    pl.run_scoped(
        body,
        *tiles,
        pltpu.VMEM((T, TILE), BF16),
        pltpu.VMEM((T, 2 * TILE), BF16),
        *[pltpu.VMEM((D, TILE), BF16)] * 2,
        pltpu.VMEM((TILE, D), BF16),
        pltpu.SemaphoreType.DMA((2, 3)),
        pltpu.SemaphoreType.DMA((5,)),
    )


def states_part(tick, dgate, dup, wg, wu, h1, y, a, rows=256):
    n = T // rows

    def body(wu_all, dg, du, sem, in_sem):
        load_up = pltpu.make_async_copy(wu, wu_all, sem)
        da = a.at[pl.ds(3 * rows, rows)]

        def at(j):
            return pl.ds(pl.multiple_of(j * rows, rows), rows)

        def ins(j):
            t = lax.rem(j, 3)
            pairs = ((dgate, dg), (dup, du), (h1, a.at[at(t)]))
            return [pltpu.make_async_copy(src.at[at(j)], dst, in_sem.at[i, t]) for i, (src, dst) in enumerate(pairs)]

        def back(j, slot):
            wide, grad = a[at(slot), :].astype(F32), da[...].astype(F32)
            scale = lax.rsqrt(jnp.mean(wide * wide, -1, keepdims=True) + 1e-6)
            inner = jnp.mean(grad * wide, -1, keepdims=True)
            dh = grad * scale - wide * (scale * scale * scale * inner)
            y[at(j), :] = (y[at(j), :].astype(F32) + dh).astype(BF16)

        def ahead(j, i):
            @pl.when(j < n - 1)
            def _():
                ins(j + 1)[i].start()

        start = ins(jnp.int32(0))
        for c in (start[0], load_up, start[1], start[2]):
            c.start()
        a[pl.ds(2 * rows, 2 * rows), :] = jnp.zeros((2 * rows, D), BF16)

        def go(j, carry):
            here = ins(j)
            here[2].wait()
            ahead(j, 2)
            here[0].wait()
            back(lax.max(j - 1, 0), lax.rem(j + 2, 3))
            by_gate = dot(dg[...], wg[...], NT)
            ahead(j, 0)
            pl.when(j == 0)(load_up.wait)
            here[1].wait()
            da[...] = (by_gate + dot(du[...], wu_all[...], NT)).astype(BF16)
            ahead(j, 1)
            tick(1, j, 0)
            return carry

        lax.fori_loop(0, n, go, 0)
        back(n - 1, (n - 1) % 3)
        tick(1, None, 0)

    pl.run_scoped(
        body,
        pltpu.VMEM((D, FF), BF16),
        *[pltpu.VMEM((rows, FF), BF16)] * 2,
        pltpu.SemaphoreType.DMA,
        pltpu.SemaphoreType.DMA((3, 3)),
    )


def down0_part(tick, p0, y, grads):
    def body(p, od, in_sem, out_sem):
        def load(j):
            s = lax.rem(j, 2)
            return pltpu.make_async_copy(p0.at[:, tile(j)], p.at[s], in_sem.at[s])

        def out(j):
            return pltpu.make_async_copy(od, grads["down"].at[tile(j)], out_sem)

        load(jnp.int32(0)).start()

        def go(j, carry):
            s = lax.rem(j, 2)
            load(j).wait()

            @pl.when(j < TILES - 1)
            def _():
                load(j + 1).start()

            @pl.when(j > 0)
            def _():
                out(j - 1).wait()

            od[...] = dot(p[s], y[...], TN).astype(BF16)
            out(j).start()
            tick(2, j, 0)
            return carry

        lax.fori_loop(0, TILES, go, 0)
        out(jnp.int32(TILES - 1)).wait()
        tick(2, None, 0)

    pl.run_scoped(
        body,
        pltpu.VMEM((2, T, TILE), BF16),
        pltpu.VMEM((TILE, D), BF16),
        pltpu.SemaphoreType.DMA((2,)),
        pltpu.SemaphoreType.DMA,
    )


def first_part(tick, a, y, wd, gate0, up0, grads):
    def body(d_tile, g, u, dgu, og, ou, in_sem, out_sem):
        def ins(j):
            s = lax.rem(j, 2)
            pairs = ((wd.at[tile(j)], d_tile.at[s]), (gate0.at[:, tile(j)], g.at[s]), (up0.at[:, tile(j)], u.at[s]))
            return [pltpu.make_async_copy(src, dst, in_sem.at[s, i]) for i, (src, dst) in enumerate(pairs)]

        def outs(j):
            pairs = ((og, grads["gate"].at[:, tile(j)]), (ou, grads["up"].at[:, tile(j)]))
            return [pltpu.make_async_copy(src, dst, out_sem.at[i]) for i, (src, dst) in enumerate(pairs)]

        for c in ins(jnp.int32(0)):
            c.start()

        def go(j, carry):
            s = lax.rem(j, 2)
            for c in ins(j):
                c.wait()

            @pl.when(j < TILES - 1)
            def _():
                for c in ins(j + 1):
                    c.start()

            for half in range(2):
                rows = pl.ds(half * HALF, HALF)
                dp = dot(y[rows, :], d_tile[s], NT).astype(BF16).astype(F32)
                _, dg_, du_ = split(g[s, rows, :], u[s, rows, :], dp)
                dgu[rows, :TILE], dgu[rows, TILE:] = dg_.astype(BF16), du_.astype(BF16)

            @pl.when(j > 0)
            def _():
                for c in outs(j - 1):
                    c.wait()

            tick(3, j, 0)
            both = dot(a[...], dgu[...], TN).astype(BF16)
            og[...], ou[...] = both[:, :TILE], both[:, TILE:]
            for c in outs(j):
                c.start()
            tick(3, j, 1)
            return carry

        lax.fori_loop(0, TILES, go, 0)
        for c in outs(jnp.int32(TILES - 1)):
            c.wait()
        tick(3, None, 0)

    pl.run_scoped(
        body,
        pltpu.VMEM((2, TILE, D), BF16),
        *[pltpu.VMEM((2, T, TILE), F32)] * 2,
        pltpu.VMEM((T, 2 * TILE), BF16),
        *[pltpu.VMEM((D, TILE), BF16)] * 2,
        pltpu.SemaphoreType.DMA((2, 3)),
        pltpu.SemaphoreType.DMA((2,)),
    )


def finish(whole, sums, m, v):
    slots, jobs = 6, 8

    def kernel(*refs):
        srcs, refs = refs[:3], refs[3:]
        small, outs, refs = refs[:9], refs[9:18], refs[18:]
        ins, results, buffers, (in_sem, out_sem, small_sem) = refs[:9], refs[9:15], refs[15:17], refs[17:]
        brought = [pltpu.make_async_copy(src, dst, small_sem.at[n]) for n, (src, dst) in enumerate(zip(small, ins))]
        taken = [pltpu.make_async_copy(src, dst, small_sem.at[n]) for n, (src, dst) in enumerate(zip(results, outs[3:]))]
        queue = [(i, n) for n in range(jobs) for i in range(3)]
        used, loads, stores = [0, 0], [], []
        for i, n in queue:
            buffer = buffers[i // 2]
            slot = used[i // 2] % buffer.shape[0]
            used[i // 2] += 1
            rows = pl.ds(n * buffer.shape[1], buffer.shape[1])
            sems = (in_sem.at[i // 2, slot], out_sem.at[i // 2, slot])
            loads.append(pltpu.make_async_copy(srcs[i].at[rows], buffer.at[slot], sems[0]))
            stores.append(pltpu.make_async_copy(buffer.at[slot], outs[i].at[rows], sems[1]))
        ahead = 2 * slots - slots // 2
        for c in (*loads[:3], *brought, *loads[3:ahead]):
            c.start()
        for n, (load, store) in enumerate(zip(loads, stores)):
            load.wait()
            store.start()
            if n >= 3 and n + ahead - 3 < len(loads):
                stores[n - 3].wait()
                loads[n + ahead - 3].start()
            if n == len(loads) // 2:
                for c in brought:
                    c.wait()
                for g, m_ref, v_ref, new_m, new_v in zip(*(ins[3 * i :][:3] for i in range(3)), results[:3], results[3:]):
                    for layer in range(2):
                        at = (slice(None), layer) if m_ref.shape[1] == 2 else (layer,)
                        grad = g[layer].astype(F32)
                        new_m[at] = 0.9 * m_ref[at] + 0.1 * grad
                        new_v[at] = 0.95 * v_ref[at] + 0.05 * grad * grad
                for c in taken:
                    c.start()
        for n, store in enumerate(stores):
            if n + ahead >= len(loads):
                store.wait()
        for c in taken:
            c.wait()

    tall = [t.reshape(-1, t.shape[-1]) for t in whole]
    shapes = [jax.ShapeDtypeStruct(t.shape, t.dtype) for t in (*tall, *m, *v)]
    hbm = pl.BlockSpec(memory_space=pl.ANY)
    room = [pltpu.VMEM(t.shape, t.dtype) for t in (*sums, *m, *v, *m, *v)]
    buffers = [pltpu.VMEM((slots, 2 * D // jobs, FF), BF16), pltpu.VMEM((slots // 2, 2 * FF // jobs, D), BF16)]
    out = pl.pallas_call(
        kernel,
        out_shape=shapes,
        in_specs=[hbm] * 12,
        out_specs=[hbm] * 9,
        scratch_shapes=room + buffers + [pltpu.SemaphoreType.DMA((2, slots))] * 2 + [pltpu.SemaphoreType.DMA((9,))],
        compiler_params=pltpu.CompilerParams(vmem_limit_bytes=67043328),
        name="finish",
    )(*tall, *sums, *m, *v)
    return [t.reshape(2, -1, t.shape[-1]) for t in out[:3]], out[3:6], out[6:]


def turned(t):
    return (*t[:2], jnp.swapaxes(t[2], 0, 1))


def step(x, dy, *arrays):
    weights, m, v = (arrays[i : i + 3] for i in (0, 3, 6))
    x, dy, m, v = x[0], dy[0], turned(m), turned(v)
    block = lax.dynamic_slice_in_dim(weights[2], lax.axis_index("dp") * 22, 22, 1)
    whole, sums = train(x, dy, weights, block, m, v)
    new_w, new_m, new_v = finish(whole, sums, m, v)
    return (*new_w, *turned(new_m), *turned(new_v))


def solution(mesh):
    P = jax.sharding.PartitionSpec
    data, state = P(("rep", "dp")), P(None, "dp")
    return jax.shard_map(
        step,
        mesh=mesh,
        in_specs=(data, data, P(), P(), P(), *[state] * 6),
        out_specs=(*[P("rep")] * 3, *[P("rep", "dp")] * 6),
        check_vma=False,
    )
```
